8 devices in a mesh: grp: 1 (over z), comp: 2 (over y), row: 4 (over x, core).
Axes of the slice: x: 2, y: 2, z: 1, core: 2. Of those that a mesh axis runs over, the one named last changes fastest.
Arguments:
- points: bfloat16 [4096, 256], P(('grp', 'row'))
- mu_init: float32 [2, 1024, 128], P(None, ('grp', 'comp'))
- logpi_init: float32 [2, 1024], P(None, ('grp', 'comp'))
- inv_temp: float32 [3], replicated
Outputs:
- output 1: float32 [2, 1024, 128], P(None, ('grp', 'comp'))
- output 2: float32 [2, 1024], P(None, ('grp', 'comp'))
- output 3: float32 [2, 4096], P(None, ('grp', 'row'))
All inputs are finite; a program needn't handle non-finite values.
Results may differ from the reference program's by a relative error of at most 0.00163705.
Values are sent between devices in bfloat16 or wider.
A program may use at most 1 GiB of HBM per device.

```python
import jax
import jax.numpy as jnp
from jax import lax

POINTS = 4096
DIM = 256
HALF = 128
COMPS = 1024
SWEEPS = 3
CLUSTERS = 16
BLOCK = 256

EPS_COUNT = 1e-6
PRIOR_ALPHA = 1e-3


def setup_inputs(seed: int = 0, part: int = 0) -> dict:
    base_key = jax.random.key(seed)
    part_key = jax.random.fold_in(base_key, part)
    key_c, key_x, key_j, key_m, key_w = jax.random.split(part_key, 5)
    key_b = jax.random.fold_in(base_key, 1000)
    centers = jax.random.normal(key_c, (2, CLUSTERS, HALF), jnp.float32)
    source = (jnp.arange(POINTS) * CLUSTERS) // POINTS
    noise_x = jax.random.normal(key_x, (2, POINTS, HALF), jnp.float32)
    pts_pair = centers[:, source, :] + 0.7 * noise_x
    points = jnp.transpose(pts_pair, (1, 0, 2)).reshape(POINTS, DIM).astype(jnp.bfloat16)
    pick_ids = jax.random.randint(key_j, (2, COMPS), 0, CLUSTERS)
    noise_m = jax.random.normal(key_m, (2, COMPS, HALF), jnp.float32)
    mu_init = centers[jnp.arange(2)[:, None], pick_ids] + 0.5 * noise_m
    raw_logit = jax.random.normal(key_w, (2, COMPS), jnp.float32)
    logpi_init = raw_logit - jax.nn.logsumexp(raw_logit, axis=1, keepdims=True)
    inv_temp = (0.5 + 1.5 * jax.random.uniform(key_b, (SWEEPS,), jnp.float32)) / HALF
    return {"points": points, "mu_init": mu_init, "logpi_init": logpi_init, "inv_temp": inv_temp}


def reference(points, mu_init, logpi_init, inv_temp):
    x_blocks = points.astype(jnp.float32).reshape(POINTS // BLOCK, BLOCK, 2, HALF)
    x_blocks = jnp.transpose(x_blocks, (0, 2, 1, 3))
    sq_blocks = jnp.sum(x_blocks * x_blocks, axis=3)

    def one_sweep(carry_in, beta_t):
        mean_vecs, log_wts = carry_in
        mu_round = mean_vecs.astype(jnp.bfloat16).astype(jnp.float32)
        mu_sq = jnp.sum(mean_vecs * mean_vecs, axis=2)

        def point_block(acc_pair, block_in):
            x_block, sq_norm = block_in
            cross_dot = jnp.einsum("snh,skh->snk", x_block, mu_round)
            logits = log_wts[:, None, :] - beta_t * (sq_norm[:, :, None] - 2.0 * cross_dot + mu_sq[:, None, :])
            row_max = jnp.max(logits, axis=2)
            shifted = jnp.exp(logits - row_max[:, :, None])
            row_sum = jnp.sum(shifted, axis=2)
            resp_f = shifted / row_sum[:, :, None]
            log_norm = row_max + jnp.log(row_sum)
            resp_round = resp_f.astype(jnp.bfloat16).astype(jnp.float32)
            stat_part = jnp.einsum("snk,snh->skh", resp_round, x_block)
            count_acc, stat_acc = acc_pair
            return (count_acc + jnp.sum(resp_f, axis=1), stat_acc + stat_part), log_norm

        zero_acc = (jnp.zeros((2, COMPS), jnp.float32), jnp.zeros((2, COMPS, HALF), jnp.float32))
        (counts, stat_sum), norm_blocks = lax.scan(point_block, zero_acc, (x_blocks, sq_blocks))
        new_means = stat_sum / (counts[:, :, None] + EPS_COUNT)
        new_logw = jnp.log((counts + PRIOR_ALPHA) / (POINTS + COMPS * PRIOR_ALPHA))
        return (new_means, new_logw), norm_blocks

    (mean_vecs, log_wts), norm_all = lax.scan(one_sweep, (mu_init, logpi_init), inv_temp)
    log_norm = jnp.transpose(norm_all[-1], (1, 0, 2)).reshape(2, POINTS)
    return mean_vecs, log_wts, log_norm
```

```python
import functools

import jax
import jax.numpy as jnp
from jax import lax
from jax.experimental import pallas as pl
from jax.experimental.pallas import tpu as pltpu
from jax.sharding import PartitionSpec as P

EPS_COUNT = 1e-6
PRIOR_ALPHA = 1e-3
LOG2E = 1.4426950408889634
LN2 = 0.6931471805599453
LANES = 128
TILE = 256

MESH = pl.DeviceIdType.MESH
F32 = jnp.float32
BF16 = jnp.bfloat16
NT = (((1,), (1,)), ((), ()))


def em_kernel(
    sweeps, total_pts, total_comp,
    temp_ref, xl_ref, mu_in, lp_in,
    mu_out, lp_out, lse_out,
    xg, mub, cc, ee, mm, stats, rr, ssum, nacc, lse2, lse_in, aux,
    s_own, r_own, s_x, r_x, s_rel, r_rel, s_st, r_st, s_lse, r_lse, s_fin, r_fin, s_frl, r_frl, s_aux, r_aux,
):
    row = lax.axis_index("row")
    y = lax.axis_index("comp")
    x = row // 2
    core = row % 2
    me = 2 * y + core
    mate = 2 * x + 1 - core
    across = 2 * (1 - x) + core
    across_mate = 2 * (1 - x) + 1 - core

    n_rows = xl_ref.shape[0]
    n_comp = mub.shape[0]
    blocks = xg.shape[0] // n_rows
    tiles = n_rows // TILE
    halves = TILE // LANES
    fit_col = pl.ds(pl.multiple_of(x * LANES, LANES), LANES)
    other_col = pl.ds(pl.multiple_of((1 - x) * LANES, LANES), LANES)
    my_comps = pl.ds(pl.multiple_of(core * n_comp, n_comp), n_comp)

    d_mate = {"row": mate}
    d_across = {"row": across}
    d_across_mate = {"row": across_mate}
    d_y = {"comp": 1 - y}
    d_y_mate = {"comp": 1 - y, "row": mate}

    def remote(src, dst, ssem, rsem, dev):
        return pltpu.make_async_remote_copy(src, dst, ssem, rsem, device_id=dev, device_id_type=MESH)

    barrier = pltpu.get_barrier_semaphore()
    for dev in (d_mate, d_across, d_across_mate, d_y, d_y_mate):
        pl.semaphore_signal(barrier, inc=1, device_id=dev, device_id_type=MESH)
    pl.semaphore_wait(barrier, 5)

    def rows_of(block, j):
        return pl.ds(pl.multiple_of(block * n_rows + j * TILE, TILE), TILE)

    own = remote(xl_ref.at[:, fit_col], xg.at[pl.ds(pl.multiple_of(row * n_rows, n_rows), n_rows), :],
                 s_own, r_own, d_mate)
    own.start()
    xs = []
    for j in range(tiles):
        c = remote(xl_ref.at[pl.ds(j * TILE, TILE), other_col], xg.at[rows_of(row, j), :], s_x.at[j], r_x.at[j], d_across)
        c.start()
        xs.append(c)

    xg[pl.ds(pl.multiple_of(row * n_rows, n_rows), n_rows), :] = xl_ref[:, fit_col]

    def set_means(sweep, mean, logw):
        mub[...] = mean.astype(BF16)
        sq = jnp.sum(mean * mean, axis=1, keepdims=True)
        cc[...] = jnp.broadcast_to(LOG2E * (logw - temp_ref[sweep] * sq), cc.shape)

    logw = jnp.transpose(jnp.broadcast_to(lp_in[pl.ds(x, 1), my_comps], (LANES, n_comp)))
    set_means(0, mu_in[x, my_comps, :], logw)

    def e_tile(sweep, block, j):
        t = block * tiles + j
        scale = (2.0 * LOG2E) * temp_ref[sweep]
        a = lax.dot_general(mub[...], xg[rows_of(block, j), :], NT, preferred_element_type=F32)
        for h in range(halves):
            z = a[:, h * LANES:(h + 1) * LANES] * scale + cc[...]
            m = jnp.max(z, axis=0, keepdims=True)
            e = jnp.exp2(z - m)
            r = jnp.sum(e, axis=0, keepdims=True)
            ee[t, :, h * LANES:(h + 1) * LANES] = e
            mm[t, h:h + 1, :] = m
            stats[sweep, me, t, h:h + 1, :] = m + jnp.log2(r)

    def st_copy(sweep, block, k):
        part = stats.at[sweep, me, pl.ds(block * tiles, tiles)]
        return remote(part, part, s_st.at[sweep, block, k], r_st.at[sweep, block, k],
                      (d_mate, d_y, d_y_mate)[k])

    def send_stats(sweep, block):
        for k in range(3):
            st_copy(sweep, block, k).start()

    def m_block(sweep, block, first):
        for k in range(3):
            st_copy(sweep, block, k).wait_recv()
        acc = None
        for j in range(tiles):
            t = block * tiles + j
            parts = [stats[sweep, d, t] for d in range(4)]
            top = jnp.maximum(jnp.maximum(parts[0], parts[1]), jnp.maximum(parts[2], parts[3]))
            tot = sum(jnp.exp2(p - top) for p in parts)
            lse = top + jnp.log2(tot)
            lse2[t] = lse
            w = jnp.exp2(mm[t] - lse)
            for h in range(halves):
                r = ee[t, :, h * LANES:(h + 1) * LANES] * w[h:h + 1, :]
                acc = r if acc is None else acc + r
                rr[:, j * TILE + h * LANES:j * TILE + (h + 1) * LANES] = r.astype(BF16)
        pts = xg[pl.ds(pl.multiple_of(block * n_rows, n_rows), n_rows), :]
        s = jnp.dot(rr[...], pts, preferred_element_type=F32)
        if first:
            ssum[...] = s
            nacc[...] = acc
        else:
            ssum[...] += s
            nacc[...] += acc

    def finish():
        n = jnp.sum(nacc[...], axis=1, keepdims=True)
        mean = ssum[...] / (n + EPS_COUNT)
        logw = jnp.log((n + PRIOR_ALPHA) / (total_pts + total_comp * PRIOR_ALPHA))
        return mean, logw

    for j in range(tiles):
        e_tile(0, row, j)
    send_stats(0, row)
    own.wait_recv()
    for j in range(tiles):
        e_tile(0, mate, j)
    send_stats(0, mate)
    relays = []
    for j in range(tiles):
        xs[j].wait_recv()
        part = xg.at[rows_of(across, j), :]
        c = remote(part, part, s_rel.at[j], r_rel.at[j], d_mate)
        c.start()
        relays.append(c)
        e_tile(0, across, j)
        if j:
            relays[j - 1].wait_recv()
            e_tile(0, across_mate, j - 1)
    send_stats(0, across)
    relays[-1].wait_recv()
    e_tile(0, across_mate, tiles - 1)
    send_stats(0, across_mate)
    for i, block in enumerate((row, mate, across, across_mate)):
        m_block(0, block, i == 0)

    for sweep in range(1, sweeps):
        mean, logw = finish()
        set_means(sweep, mean, logw)
        for block in range(blocks):
            for j in range(tiles):
                e_tile(sweep, block, j)
            send_stats(sweep, block)
        for block in range(blocks):
            m_block(sweep, block, block == 0)

    last = remote(lse2.at[pl.ds(across * tiles, tiles)], lse_in, s_lse, r_lse, d_across)
    last.start()
    mean, logw = finish()
    mu_out[x, my_comps, :] = mean
    parts = 2
    step = n_comp // parts
    fins = []
    for p in range(parts):
        piece = mu_out.at[x, pl.ds(pl.multiple_of(core * n_comp + p * step, step), step), :]
        c = remote(piece, piece, s_fin.at[0, p], r_fin.at[0, p], d_across)
        c.start()
        fins.append(c)
    piece = mu_out.at[x, my_comps, :]
    to_mate = remote(piece, piece, s_fin.at[1, 0], r_fin.at[1, 0], d_mate)
    to_mate.start()
    flat = jnp.transpose(jnp.broadcast_to(logw, (n_comp, LANES)))[0:1, :]
    for h in range(n_comp // LANES):
        aux[row, h:h + 1, :] = flat[:, h * LANES:(h + 1) * LANES]
    auxs = []
    for k, dev in enumerate((d_mate, d_across, d_across_mate)):
        c = remote(aux.at[row], aux.at[row], s_aux.at[k], r_aux.at[k], dev)
        c.start()
        auxs.append(c)

    ones = jnp.ones((8, LANES), BF16)
    last.wait_recv()
    for s in range(2):
        xf = xl_ref[:, s * LANES:(s + 1) * LANES].astype(F32)
        xx = xf * xf
        hi = xx.astype(BF16)
        lo = (xx - hi.astype(F32)).astype(BF16)
        sq = lax.dot_general(ones, hi, NT, preferred_element_type=F32)
        sq = sq + lax.dot_general(ones, lo, NT, preferred_element_type=F32)
        for j in range(tiles):
            val = jnp.where(x == s, lse2[row * tiles + j], lse_in[j])
            for h in range(halves):
                at = slice(j * TILE + h * LANES, j * TILE + (h + 1) * LANES)
                lse_out[s:s + 1, at] = val[h:h + 1, :] * LN2 - temp_ref[sweeps - 1] * sq[0:1, at]

    frels = []
    for p in range(parts):
        fins[p].wait_recv()
        piece = mu_out.at[1 - x, pl.ds(pl.multiple_of(core * n_comp + p * step, step), step), :]
        c = remote(piece, piece, s_frl.at[p], r_frl.at[p], d_mate)
        c.start()
        frels.append(c)
    for c in auxs:
        c.wait_recv()
    for b in range(blocks):
        for h in range(n_comp // LANES):
            at = (b % 2) * n_comp + h * LANES
            lp_out[b // 2:b // 2 + 1, at:at + LANES] = aux[b, h:h + 1, :]
    to_mate.wait_recv()
    for c in frels:
        c.wait_recv()

    for c in [own, to_mate, last] + xs + relays + fins + frels + auxs:
        c.wait_send()
    for sweep in range(sweeps):
        for block in range(blocks):
            for k in range(3):
                st_copy(sweep, block, k).wait_send()


def solution(mesh):
    rows_size = mesh.shape["row"]
    comp_size = mesh.shape["comp"]

    def local_fit(x_local, mu_init, logpi_init, inv_temp):
        n_rows = x_local.shape[0]
        half = x_local.shape[1] // 2
        n_half = mu_init.shape[1]
        n_comp = n_half // 2
        sweeps = inv_temp.shape[0]
        total_pts = n_rows * rows_size
        n_tiles = total_pts // TILE
        tiles = n_rows // TILE
        halves = TILE // LANES
        vmem = pl.BlockSpec(memory_space=pltpu.VMEM)
        dma = pltpu.SemaphoreType.DMA
        return pl.pallas_call(
            functools.partial(em_kernel, sweeps, total_pts, n_half * comp_size),
            out_shape=(
                jax.ShapeDtypeStruct(mu_init.shape, F32),
                jax.ShapeDtypeStruct(logpi_init.shape, F32),
                jax.ShapeDtypeStruct((2, n_rows), F32),
            ),
            in_specs=[pl.BlockSpec(memory_space=pltpu.SMEM), vmem, vmem, vmem],
            out_specs=(vmem, vmem, vmem),
            scratch_shapes=[
                pltpu.VMEM((total_pts, half), BF16),
                pltpu.VMEM((n_comp, half), BF16),
                pltpu.VMEM((n_comp, LANES), F32),
                pltpu.VMEM((n_tiles, n_comp, TILE), F32),
                pltpu.VMEM((n_tiles, halves, LANES), F32),
                pltpu.VMEM((sweeps, 4, n_tiles, halves, LANES), F32),
                pltpu.VMEM((n_comp, n_rows), BF16),
                pltpu.VMEM((n_comp, half), F32),
                pltpu.VMEM((n_comp, LANES), F32),
                pltpu.VMEM((n_tiles, halves, LANES), F32),
                pltpu.VMEM((tiles, halves, LANES), F32),
                pltpu.VMEM((rows_size, n_comp // LANES, LANES), F32),
                dma, dma, dma((tiles,)), dma((tiles,)), dma((tiles,)), dma((tiles,)),
                dma((sweeps, rows_size, 3)), dma((sweeps, rows_size, 3)),
                dma, dma, dma((2, 2)), dma((2, 2)), dma((2,)), dma((2,)), dma((3,)), dma((3,)),
            ],
            compiler_params=pltpu.CompilerParams(collective_id=0, has_side_effects=True),
        )(inv_temp, x_local, mu_init, logpi_init)

    return jax.shard_map(
        local_fit,
        mesh=mesh,
        in_specs=(P(("grp", "row"), None), P(None, ("grp", "comp"), None), P(None, ("grp", "comp")), P()),
        out_specs=(P(None, ("grp", "comp"), None), P(None, ("grp", "comp")), P(None, ("grp", "row"))),
        check_vma=False,
    )
```

```python
import functools

import jax
import jax.numpy as jnp
from jax import lax
from jax.experimental import pallas as pl
from jax.experimental.pallas import tpu as pltpu
from jax.sharding import PartitionSpec as P

EPS_COUNT = 1e-6
PRIOR_ALPHA = 1e-3
LOG2E = 1.4426950408889634
LN2 = 0.6931471805599453
LANES = 128
TILE = 256
PIECES = 4

MESH = pl.DeviceIdType.MESH
F32 = jnp.float32
BF16 = jnp.bfloat16
NT = (((1,), (1,)), ((), ()))


def em_kernel(
    sweeps, total_pts, total_comp,
    temp_in, x_in, mu_in, lp_in,
    mu_out, lp_out, lse_out,
    temp_ref, xo, xg, mu0, lp0, mub, cc, ee, mm, stats, rr, ssum, nacc, lse2, lse_in, aux,
    s_in, s_own, r_own, s_x, r_x, s_rel, r_rel, s_st, r_st, s_lse, r_lse,
    s_fin, r_fin, s_mate, r_mate, s_frl, r_frl, s_aux, r_aux,
):
    row = lax.axis_index("row")
    y = lax.axis_index("comp")
    x = row // 2
    core = row % 2
    me = 2 * y + core
    mate = 2 * x + 1 - core
    across = 2 * (1 - x) + core
    across_mate = 2 * (1 - x) + 1 - core

    n_rows = xo.shape[0]
    n_comp = mub.shape[0]
    blocks = xg.shape[0] // n_rows
    tiles = n_rows // TILE
    halves = TILE // LANES
    fit_col = pl.ds(pl.multiple_of(x * LANES, LANES), LANES)
    other_col = pl.ds(pl.multiple_of((1 - x) * LANES, LANES), LANES)
    my_comps = pl.ds(pl.multiple_of(core * n_comp, n_comp), n_comp)
    my_rows = pl.ds(pl.multiple_of(row * n_rows, n_rows), n_rows)

    d_mate = {"row": mate}
    d_across = {"row": across}
    d_across_mate = {"row": across_mate}
    d_y = {"comp": 1 - y}
    d_y_mate = {"comp": 1 - y, "row": mate}

    def drain(ref, sem):
        pltpu.make_async_copy(ref, ref, sem).wait()

    def remote(src, dst, ssem, rsem, dev):
        return pltpu.make_async_remote_copy(src, dst, ssem, rsem, device_id=dev, device_id_type=MESH)

    loads = [
        pltpu.make_async_copy(src, dst, s_in.at[i])
        for i, (src, dst) in enumerate((
            (x_in.at[:, other_col], xo),
            (x_in.at[:, fit_col], xg.at[my_rows, :]),
            (mu_in.at[x, my_comps, :], mu0),
            (lp_in, lp0),
            (temp_in, temp_ref),
        ))
    ]
    barrier = pltpu.get_barrier_semaphore()
    for dev in (d_mate, d_across, d_across_mate, d_y, d_y_mate):
        pl.semaphore_signal(barrier, inc=1, device_id=dev, device_id_type=MESH)
    for c in loads:
        c.start()
    with jax.named_scope("barrier"):
        pl.semaphore_wait(barrier, 5)
    with jax.named_scope("loads"):
        for c in loads:
            c.wait()

    def rows_of(block, j):
        return pl.ds(pl.multiple_of(block * n_rows + j * TILE, TILE), TILE)

    xs = []
    for j in range(tiles):
        c = remote(xo.at[pl.ds(j * TILE, TILE), :], xg.at[rows_of(row, j), :], s_x, r_x.at[j], d_across)
        c.start()
        xs.append(c)
    own = remote(xg.at[my_rows, :], xg.at[my_rows, :], s_own, r_own, d_mate)
    own.start()

    def set_means(sweep, mean, logw):
        mub[...] = mean.astype(BF16)
        sq = jnp.sum(mean * mean, axis=1, keepdims=True)
        cc[...] = jnp.broadcast_to(LOG2E * (logw - temp_ref[sweep] * sq), cc.shape)

    logw = jnp.transpose(jnp.broadcast_to(lp0[pl.ds(x, 1), my_comps], (LANES, n_comp)))
    set_means(0, mu0[...], logw)

    def cross(block, j):
        return lax.dot_general(mub[...], xg[rows_of(block, j), :], NT, preferred_element_type=F32)

    def e_tile(sweep, block, j, a):
        t = block * tiles + j
        scale = (2.0 * LOG2E) * temp_ref[sweep]
        for h in range(halves):
            z = a[:, h * LANES:(h + 1) * LANES] * scale + cc[...]
            m = jnp.max(z, axis=0, keepdims=True)
            e = jnp.exp2(z - m)
            r = jnp.sum(e, axis=0, keepdims=True)
            ee[t, :, h * LANES:(h + 1) * LANES] = e
            mm[t, h:h + 1, :] = m
            stats[sweep, me, t, h:h + 1, :] = m + jnp.log2(r)

    def st_copy(sweep, block, k):
        part = stats.at[sweep, me, pl.ds(block * tiles, tiles)]
        return remote(part, part, s_st, r_st.at[sweep, block], (d_mate, d_y, d_y_mate)[k])

    def send_stats(sweep, block):
        for k in (1, 2, 0):
            st_copy(sweep, block, k).start()

    def e_blocks(sweep, todo):
        order = [(block, j) for block in todo for j in range(tiles)]
        ahead = cross(*order[0])
        for i, (block, j) in enumerate(order):
            a = ahead
            if i + 1 < len(order):
                ahead = cross(*order[i + 1])
            e_tile(sweep, block, j, a)
            if j == tiles - 1:
                send_stats(sweep, block)

    def m_blocks(sweep, todo, first):
        with jax.named_scope("stwait"):
            for block in todo:
                drain(stats.at[sweep, pl.ds(0, 3), pl.ds(block * tiles, tiles)], r_st.at[sweep, block])
        with jax.named_scope("mblock"):
            m_blocks_(sweep, todo, first)

    def m_blocks_(sweep, todo, first):
        for i, block in enumerate(todo):
            ws = []
            for j in range(tiles):
                t = block * tiles + j
                parts = [stats[sweep, d, t] for d in range(4)]
                top = jnp.maximum(jnp.maximum(parts[0], parts[1]), jnp.maximum(parts[2], parts[3]))
                tot = (jnp.exp2(parts[0] - top) + jnp.exp2(parts[1] - top)) + (
                    jnp.exp2(parts[2] - top) + jnp.exp2(parts[3] - top))
                lse = top + jnp.log2(tot)
                lse2[t] = lse
                w = jnp.exp2(mm[t] - lse)
                ws += [w[h:h + 1, :] for h in range(halves)]
            for k in range(0, n_comp, 16):
                acc = None if first and i == 0 else nacc[k:k + 16, :]
                for v, w in enumerate(ws):
                    r = ee[block * tiles + v // halves, k:k + 16, (v % halves) * LANES:(v % halves + 1) * LANES] * w
                    acc = r if acc is None else acc + r
                    rr[block, k:k + 16, v * LANES:(v + 1) * LANES] = r.astype(BF16)
                nacc[k:k + 16, :] = acc
            pts = xg[pl.ds(pl.multiple_of(block * n_rows, n_rows), n_rows), :]
            s = jnp.dot(rr[block], pts, preferred_element_type=F32)
            if first and i == 0:
                ssum[...] = s
            else:
                ssum[...] += s

    def finish():
        n = jnp.sum(nacc[...], axis=1, keepdims=True)
        mean = ssum[...] / (n + EPS_COUNT)
        logw = jnp.log((n + PRIOR_ALPHA) / (total_pts + total_comp * PRIOR_ALPHA))
        return mean, logw

    with jax.named_scope("e_own"):
        e_blocks(0, (row,))
    with jax.named_scope("w_own"):
        own.wait_recv()
    with jax.named_scope("e_mate"):
        e_blocks(0, (mate,))
    relays = []
    for j in range(tiles):
        with jax.named_scope(f"w_x{j}"):
            xs[j].wait_recv()
        part = xg.at[rows_of(across, j), :]
        c = remote(part, part, s_rel, r_rel.at[j], d_mate)
        c.start()
        relays.append(c)
        e_tile(0, across, j, cross(across, j))
        if j == tiles - 1:
            send_stats(0, across)
        if j:
            with jax.named_scope(f"w_rel{j}"):
                relays[j - 1].wait_recv()
            e_tile(0, across_mate, j - 1, cross(across_mate, j - 1))
        if j == 2:
            m_blocks(0, (row, mate), True)
    with jax.named_scope("w_rel4"):
        relays[-1].wait_recv()
    e_tile(0, across_mate, tiles - 1, cross(across_mate, tiles - 1))
    send_stats(0, across_mate)
    m_blocks(0, (across,), False)
    m_blocks(0, (across_mate,), False)

    for sweep in range(1, sweeps):
        with jax.named_scope("finish"):
            mean, logw = finish()
            set_means(sweep, mean, logw)
        with jax.named_scope("esweep"):
            e_blocks(sweep, range(blocks))
        for block in range(blocks):
            m_blocks(sweep, (block,), block == 0)

    mean, logw = finish()
    mu_out[x, my_comps, :] = mean
    step = n_comp // PIECES
    fins = []

    def piece(fit, p):
        return mu_out.at[fit, pl.ds(pl.multiple_of(core * n_comp + p * step, step), step), :]

    for p in range(PIECES):
        c = remote(piece(x, p), piece(x, p), s_fin, r_fin.at[p], d_across)
        c.start()
        fins.append(c)
    part = mu_out.at[x, my_comps, :]
    to_mate = remote(part, part, s_mate, r_mate, d_mate)
    to_mate.start()
    last = remote(lse2.at[pl.ds(across * tiles, tiles)], lse_in, s_lse, r_lse, d_across)
    last.start()
    flat = jnp.transpose(jnp.broadcast_to(logw, (n_comp, LANES)))[0:1, :]
    for h in range(n_comp // LANES):
        aux[row, h:h + 1, :] = flat[:, h * LANES:(h + 1) * LANES]
    auxs = []
    for k, dev in enumerate((d_mate, d_across, d_across_mate)):
        c = remote(aux.at[row], aux.at[row], s_aux, r_aux, dev)
        c.start()
        auxs.append(c)

    ones = jnp.ones((8, LANES), BF16)

    def sq_rows(pts):
        xf = pts.astype(F32)
        xx = xf * xf
        hi = xx.astype(BF16)
        lo = (xx - hi.astype(F32)).astype(BF16)
        sq = lax.dot_general(ones, hi, NT, preferred_element_type=F32)
        return sq + lax.dot_general(ones, lo, NT, preferred_element_type=F32)

    def write_lse(sq_own, sq_other):
        for s in range(2):
            sq = jnp.where(x == s, sq_own, sq_other)
            for j in range(tiles):
                val = jnp.where(x == s, lse2[row * tiles + j], lse_in[j])
                for h in range(halves):
                    at = slice(j * TILE + h * LANES, j * TILE + (h + 1) * LANES)
                    lse_out[s:s + 1, at] = val[h:h + 1, :] * LN2 - temp_ref[sweeps - 1] * sq[0:1, at]

    with jax.named_scope("lse"):
        sq_own = sq_rows(xg[my_rows, :])
        sq_other = sq_rows(xo[...])
    frels = []
    for p in range(PIECES):
        with jax.named_scope(f"w_fin{p}"):
            fins[p].wait_recv()
        c = remote(piece(1 - x, p), piece(1 - x, p), s_frl, r_frl, d_mate)
        c.start()
        frels.append(c)
    with jax.named_scope("w_last"):
        last.wait_recv()
    write_lse(sq_own, sq_other)
    drain(aux.at[pl.ds(0, 3)], r_aux)
    for b in range(blocks):
        for h in range(n_comp // LANES):
            at = (b % 2) * n_comp + h * LANES
            lp_out[b // 2:b // 2 + 1, at:at + LANES] = aux[b, h:h + 1, :]
    with jax.named_scope("w_frel"):
        to_mate.wait_recv()
        drain(ssum, r_frl)
    with jax.named_scope("w_sends"):
        for c in (own, to_mate, last):
            c.wait_send()
        drain(xo, s_x)
        drain(xo, s_rel)
        drain(ssum, s_fin)
        drain(ssum, s_frl)
        drain(aux.at[pl.ds(0, 3)], s_aux)
        drain(stats.at[:, pl.ds(0, 3)], s_st)


def store_kernel(a, b, c, a_out, b_out, c_out, sem):
    copies = [
        pltpu.make_async_copy(src, dst, sem.at[i])
        for i, (src, dst) in enumerate(((a, a_out), (b, b_out), (c, c_out)))
    ]
    for c in copies:
        c.start()
    for c in copies:
        c.wait()


def solution(mesh):
    rows_size = mesh.shape["row"]
    comp_size = mesh.shape["comp"]

    def local_fit(x_local, mu_init, logpi_init, inv_temp):
        n_rows = x_local.shape[0]
        half = x_local.shape[1] // 2
        n_half = mu_init.shape[1]
        n_comp = n_half // 2
        sweeps = inv_temp.shape[0]
        total_pts = n_rows * rows_size
        n_tiles = total_pts // TILE
        tiles = n_rows // TILE
        halves = TILE // LANES
        vmem = pl.BlockSpec(memory_space=pltpu.VMEM)
        hbm = pl.BlockSpec(memory_space=pl.ANY)
        dma = pltpu.SemaphoreType.DMA
        outs = pl.pallas_call(
            functools.partial(em_kernel, sweeps, total_pts, n_half * comp_size),
            out_shape=(
                pltpu.VMEM(mu_init.shape, F32),
                pltpu.VMEM(logpi_init.shape, F32),
                pltpu.VMEM((2, n_rows), F32),
            ),
            in_specs=[hbm] * 4,
            out_specs=(vmem, vmem, vmem),
            scratch_shapes=[
                pltpu.SMEM((sweeps,), F32),
                pltpu.VMEM((n_rows, half), BF16),
                pltpu.VMEM((total_pts, half), BF16),
                pltpu.VMEM((n_comp, half), F32),
                pltpu.VMEM(logpi_init.shape, F32),
                pltpu.VMEM((n_comp, half), BF16),
                pltpu.VMEM((n_comp, LANES), F32),
                pltpu.VMEM((n_tiles, n_comp, TILE), F32),
                pltpu.VMEM((n_tiles, halves, LANES), F32),
                pltpu.VMEM((sweeps, 4, n_tiles, halves, LANES), F32),
                pltpu.VMEM((rows_size, n_comp, n_rows), BF16),
                pltpu.VMEM((n_comp, half), F32),
                pltpu.VMEM((n_comp, LANES), F32),
                pltpu.VMEM((n_tiles, halves, LANES), F32),
                pltpu.VMEM((tiles, halves, LANES), F32),
                pltpu.VMEM((rows_size, n_comp // LANES, LANES), F32),
                dma((5,)), dma, dma, dma, dma((tiles,)), dma, dma((tiles,)), dma, dma((sweeps, rows_size)), dma, dma,
                dma, dma((PIECES,)), dma, dma, dma, dma, dma, dma,
            ],
            compiler_params=pltpu.CompilerParams(collective_id=0, has_side_effects=True),
        )(inv_temp, x_local, mu_init, logpi_init)
        outs = [pltpu.with_memory_space_constraint(o, pltpu.VMEM) for o in outs]
        return pl.pallas_call(
            store_kernel,
            out_shape=tuple(jax.ShapeDtypeStruct(o.shape, F32) for o in outs),
            in_specs=[vmem] * 3,
            out_specs=(hbm, hbm, hbm),
            scratch_shapes=[dma((3,))],
        )(*outs)

    return jax.shard_map(
        local_fit,
        mesh=mesh,
        in_specs=(P(("grp", "row"), None), P(None, ("grp", "comp"), None), P(None, ("grp", "comp")), P()),
        out_specs=(P(None, ("grp", "comp"), None), P(None, ("grp", "comp")), P(None, ("grp", "row"))),
        check_vma=False,
    )
```

```python
import functools

import jax
import jax.numpy as jnp
from jax import lax
from jax.experimental import pallas as pl
from jax.experimental.pallas import tpu as pltpu
from jax.sharding import PartitionSpec as P

EPS_COUNT = 1e-6
PRIOR_ALPHA = 1e-3
LOG2E = 1.4426950408889634
LN2 = 0.6931471805599453
LANES = 128
TILE = 256
PIECES = 4

MESH = pl.DeviceIdType.MESH
F32 = jnp.float32
BF16 = jnp.bfloat16
NT = (((1,), (1,)), ((), ()))


def em_kernel(
    sweeps, total_pts, total_comp,
    temp_in, x_in, mu_in, lp_in,
    mu_out, lp_out, lse_out,
    temp_ref, xo, xg, mu0, lp0, mub0, cc0, stats0, part, inbox, xsend, xin, nsend, nin,
    mub, cc, ee, mm, stats, rr, ssum, nacc, lse2, lse_in, aux,
    s_in, s_own, r_own, s_x, r_x, s_rel, r_rel, s_st0, r_st0, s_part, r_part, s_xs, r_xs, s_n, r_n,
    s_st, r_st, s_lse, r_lse, s_fin, r_fin, s_mate, r_mate, s_frl, r_frl, s_aux, r_aux,
):
    row = lax.axis_index("row")
    y = lax.axis_index("comp")
    x = row // 2
    core = row % 2
    me = 2 * y + core
    mate = 2 * x + 1 - core
    across = 2 * (1 - x) + core
    across_mate = 2 * (1 - x) + 1 - core

    n_rows = xo.shape[0]
    n_comp = mub.shape[0]
    blocks = xg.shape[0] // n_rows
    tiles = n_rows // TILE
    halves = TILE // LANES
    fit_col = pl.ds(pl.multiple_of(x * LANES, LANES), LANES)
    other_col = pl.ds(pl.multiple_of((1 - x) * LANES, LANES), LANES)
    my_comps = pl.ds(pl.multiple_of(core * n_comp, n_comp), n_comp)
    mates_comps = pl.ds(pl.multiple_of((1 - core) * n_comp, n_comp), n_comp)
    my_rows = pl.ds(pl.multiple_of(row * n_rows, n_rows), n_rows)

    d_mate = {"row": mate}
    d_across = {"row": across}
    d_across_mate = {"row": across_mate}
    d_y = {"comp": 1 - y}
    d_y_mate = {"comp": 1 - y, "row": mate}

    def drain(ref, sem):
        pltpu.make_async_copy(ref, ref, sem).wait()

    def remote(src, dst, ssem, rsem, dev):
        return pltpu.make_async_remote_copy(src, dst, ssem, rsem, device_id=dev, device_id_type=MESH)

    loads = [
        pltpu.make_async_copy(src, dst, s_in.at[i])
        for i, (src, dst) in enumerate((
            (x_in.at[:, other_col], xo),
            (x_in.at[:, fit_col], xg.at[my_rows, :]),
            (mu_in, mu0),
            (lp_in, lp0),
            (temp_in, temp_ref),
        ))
    ]
    barrier = pltpu.get_barrier_semaphore()
    for dev in (d_mate, d_across, d_across_mate, d_y, d_y_mate):
        pl.semaphore_signal(barrier, inc=1, device_id=dev, device_id_type=MESH)
    for c in loads:
        c.start()
    with jax.named_scope("barrier"):
        pl.semaphore_wait(barrier, 5)
    with jax.named_scope("loads"):
        for c in loads:
            c.wait()

    def rows_of(block, j):
        return pl.ds(pl.multiple_of(block * n_rows + j * TILE, TILE), TILE)

    xs = [
        remote(xo.at[pl.ds(j * TILE, TILE), :], xg.at[rows_of(row, j), :], s_x, r_x.at[j], d_across)
        for j in range(tiles)
    ]
    relays = [
        remote(xg.at[rows_of(across, j), :], xg.at[rows_of(across, j), :], s_rel, r_rel.at[j], d_mate)
        for j in range(tiles)
    ]
    own = remote(xg.at[my_rows, :], xg.at[my_rows, :], s_own, r_own, d_mate)
    for c in xs[:-1]:
        c.start()
    own.start()

    def means_to(sweep, mean, logw, mub_at, cc_at):
        mub_at[...] = mean.astype(BF16)
        sq = jnp.sum(mean * mean, axis=1, keepdims=True)
        cc_at[...] = jnp.broadcast_to(LOG2E * (logw - temp_ref[sweep] * sq), cc_at.shape)

    def column(flat):
        return jnp.transpose(jnp.broadcast_to(flat, (LANES, n_comp)))

    def e_tile(sweep, t, a, cc_at, stat):
        scale = (2.0 * LOG2E) * temp_ref[sweep]
        for h in range(halves):
            z = a[:, h * LANES:(h + 1) * LANES] * scale + cc_at[...]
            m = jnp.max(z, axis=0, keepdims=True)
            e = jnp.exp2(z - m)
            r = jnp.sum(e, axis=0, keepdims=True)
            ee[t, :, h * LANES:(h + 1) * LANES] = e
            mm[t, h:h + 1, :] = m
            stat[h:h + 1, :] = m + jnp.log2(r)

    def lse_of(parts):
        top = jnp.maximum(jnp.maximum(parts[0], parts[1]), jnp.maximum(parts[2], parts[3]))
        tot = (jnp.exp2(parts[0] - top) + jnp.exp2(parts[1] - top)) + (
            jnp.exp2(parts[2] - top) + jnp.exp2(parts[3] - top))
        return top + jnp.log2(tot)

    def m_region(lses, base, pts, slot, n_at, s_at, first):
        ws = []
        for j in range(tiles):
            w = jnp.exp2(mm[base + j] - lses[j])
            ws += [w[h:h + 1, :] for h in range(halves)]
        for k in range(0, n_comp, 16):
            acc = None if first else n_at[k:k + 16, :]
            for v, w in enumerate(ws):
                r = ee[base + v // halves, k:k + 16, (v % halves) * LANES:(v % halves + 1) * LANES] * w
                acc = r if acc is None else acc + r
                rr[slot, k:k + 16, v * LANES:(v + 1) * LANES] = r.astype(BF16)
            n_at[k:k + 16, :] = acc
        s = jnp.dot(rr[slot], pts, preferred_element_type=F32)
        if first:
            s_at[...] = s
        else:
            s_at[...] += s

    def cross0(slot, j):
        pts = xg[rows_of(row, j), :] if slot // 2 else xo[pl.ds(j * TILE, TILE), :]
        return lax.dot_general(mub0[slot], pts, NT, preferred_element_type=F32)

    def st0_copy(fo):
        at = stats0.at[fo, pl.ds(2 * y, 2)]
        return remote(at, at, s_st0, r_st0.at[fo], d_y)

    for fo, fit in enumerate((1 - x, x)):
        with jax.named_scope(f"set0_{fo}"):
            for qo, comps in enumerate((mates_comps, my_comps)):
                slot = 2 * fo + qo
                means_to(0, mu0[fit, comps, :], column(lp0[pl.ds(fit, 1), comps]), mub0.at[slot], cc0.at[slot])
        with jax.named_scope(f"e0_{fo}"):
            order = [(2 * fo + qo, j) for qo in range(2) for j in range(tiles)]
            ahead = cross0(*order[0])
            for i, (slot, j) in enumerate(order):
                a = ahead
                if i + 1 < len(order):
                    ahead = cross0(*order[i + 1])
                e_tile(0, slot * tiles + j, a, cc0.at[slot], stats0.at[fo, 2 * y + slot % 2, j])
        st0_copy(fo).start()

    def part_copy(fo, k):
        return remote(part.at[2 * fo, k], inbox.at[fo, k], s_part, r_part.at[fo, k], d_mate)

    def m0(fo, qo):
        slot = 2 * fo + qo
        lses = [lse_of([stats0[fo, d, j] for d in range(4)]) for j in range(tiles)]
        pts = xg[my_rows, :] if fo else xo[...]
        m_region(lses, slot * tiles, pts, slot, part.at[slot, 1], part.at[slot, 0], True)

    step = n_comp // PIECES
    with jax.named_scope("w_st0_0"):
        st0_copy(0).wait_recv()
    with jax.named_scope("m0_0"):
        m0(0, 0)
    for k in range(2):
        part_copy(0, k).start()
    with jax.named_scope("m0_1"):
        m0(0, 1)
    with jax.named_scope("w_part0"):
        part_copy(0, 0).wait_recv()
    sums = []
    for p in range(PIECES):
        at = pl.ds(p * step, step)
        xsend[at, :] = part[1, 0, at, :] + inbox[0, 0, at, :]
        c = remote(xsend.at[at, :], xin.at[at, :], s_xs, r_xs, d_across)
        c.start()
        sums.append(c)
    part_copy(0, 1).wait_recv()
    flat = jnp.sum(jnp.transpose(part[1, 1] + inbox[0, 1]), axis=0, keepdims=True)
    for h in range(n_comp // LANES):
        nsend[h:h + 1, :] = flat[:, h * LANES:(h + 1) * LANES]
    counts = remote(nsend, nin, s_n, r_n, d_across)
    counts.start()
    xs[-1].start()
    with jax.named_scope("w_st0_1"):
        st0_copy(1).wait_recv()
    with jax.named_scope("m0_2"):
        m0(1, 0)
    for k in range(2):
        part_copy(1, k).start()
    with jax.named_scope("m0_3"):
        m0(1, 1)
    for j in range(tiles - 1):
        with jax.named_scope(f"w_x{j}"):
            xs[j].wait_recv()
        relays[j].start()
    with jax.named_scope("w_part1"):
        for k in range(2):
            part_copy(1, k).wait_recv()
    with jax.named_scope("w_xin"):
        counts.wait_recv()
        drain(xsend, r_xs)
    n_across = column(jnp.concatenate([nin[h:h + 1, :] for h in range(n_comp // LANES)], axis=1))
    ssum[...] = part[3, 0] + inbox[1, 0] + xin[...]
    n_first = jnp.sum(part[3, 1] + inbox[1, 1], axis=1, keepdims=True) + n_across

    def cross(block, j):
        return lax.dot_general(mub[...], xg[rows_of(block, j), :], NT, preferred_element_type=F32)

    def st_copy(sweep, block, k):
        part = stats.at[sweep - 1, me, pl.ds(block * tiles, tiles)]
        return remote(part, part, s_st, r_st.at[sweep - 1, block], (d_mate, d_y, d_y_mate)[k])

    def send_stats(sweep, block):
        for k in (1, 2, 0):
            st_copy(sweep, block, k).start()

    def e_blocks(sweep, todo):
        order = [(block, j) for block in todo for j in range(tiles)]
        ahead = cross(*order[0])
        for i, (block, j) in enumerate(order):
            a = ahead
            if i + 1 < len(order):
                ahead = cross(*order[i + 1])
            t = block * tiles + j
            e_tile(sweep, t, a, cc, stats.at[sweep - 1, me, t])
            if j == tiles - 1:
                send_stats(sweep, block)

    def m_block(sweep, block, first):
        with jax.named_scope("stwait"):
            drain(stats.at[sweep - 1, pl.ds(0, 3), pl.ds(block * tiles, tiles)], r_st.at[sweep - 1, block])
        with jax.named_scope("mblock"):
            lses = []
            for j in range(tiles):
                t = block * tiles + j
                lses.append(lse_of([stats[sweep - 1, d, t] for d in range(4)]))
                lse2[t] = lses[-1]
            pts = xg[pl.ds(pl.multiple_of(block * n_rows, n_rows), n_rows), :]
            m_region(lses, block * tiles, pts, block, nacc, ssum, first)

    def finish(n):
        mean = ssum[...] / (n + EPS_COUNT)
        logw = jnp.log((n + PRIOR_ALPHA) / (total_pts + total_comp * PRIOR_ALPHA))
        return mean, logw

    with jax.named_scope("finish"):
        mean, logw = finish(n_first)
        means_to(1, mean, logw, mub, cc)
    for sweep in range(1, sweeps):
        if sweep == 1:
            with jax.named_scope("e_row"):
                e_blocks(1, (row,))
            with jax.named_scope("w_own"):
                own.wait_recv()
            with jax.named_scope("e_mate"):
                e_blocks(1, (mate,))
            with jax.named_scope("w_x3"):
                xs[-1].wait_recv()
            relays[-1].start()
            with jax.named_scope("e_across"):
                e_blocks(1, (across,))
            with jax.named_scope("w_rel"):
                for c in relays:
                    c.wait_recv()
            with jax.named_scope("e_across_mate"):
                e_blocks(1, (across_mate,))
            order = (row, mate, across, across_mate)
        else:
            with jax.named_scope("esweep"):
                e_blocks(sweep, range(blocks))
            order = range(blocks)
        for i, block in enumerate(order):
            m_block(sweep, block, i == 0)
        with jax.named_scope("finish"):
            mean, logw = finish(jnp.sum(nacc[...], axis=1, keepdims=True))
            if sweep + 1 < sweeps:
                means_to(sweep + 1, mean, logw, mub, cc)

    mu_out[x, my_comps, :] = mean
    fins = []

    def piece(fit, p):
        return mu_out.at[fit, pl.ds(pl.multiple_of(core * n_comp + p * step, step), step), :]

    for p in range(PIECES):
        c = remote(piece(x, p), piece(x, p), s_fin, r_fin.at[p], d_across)
        c.start()
        fins.append(c)
    whole = mu_out.at[x, my_comps, :]
    to_mate = remote(whole, whole, s_mate, r_mate, d_mate)
    to_mate.start()
    last = remote(lse2.at[pl.ds(across * tiles, tiles)], lse_in, s_lse, r_lse, d_across)
    last.start()
    flat = jnp.transpose(jnp.broadcast_to(logw, (n_comp, LANES)))[0:1, :]
    for h in range(n_comp // LANES):
        aux[row, h:h + 1, :] = flat[:, h * LANES:(h + 1) * LANES]
    auxs = []
    for k, dev in enumerate((d_mate, d_across, d_across_mate)):
        c = remote(aux.at[row], aux.at[row], s_aux, r_aux, dev)
        c.start()
        auxs.append(c)

    ones = jnp.ones((8, LANES), BF16)

    def sq_rows(pts):
        xf = pts.astype(F32)
        xx = xf * xf
        hi = xx.astype(BF16)
        lo = (xx - hi.astype(F32)).astype(BF16)
        sq = lax.dot_general(ones, hi, NT, preferred_element_type=F32)
        return sq + lax.dot_general(ones, lo, NT, preferred_element_type=F32)

    def write_lse(sq_own, sq_other):
        for s in range(2):
            sq = jnp.where(x == s, sq_own, sq_other)
            for j in range(tiles):
                val = jnp.where(x == s, lse2[row * tiles + j], lse_in[j])
                for h in range(halves):
                    at = slice(j * TILE + h * LANES, j * TILE + (h + 1) * LANES)
                    lse_out[s:s + 1, at] = val[h:h + 1, :] * LN2 - temp_ref[sweeps - 1] * sq[0:1, at]

    with jax.named_scope("lse"):
        sq_own = sq_rows(xg[my_rows, :])
        sq_other = sq_rows(xo[...])
    frels = []
    for p in range(PIECES):
        with jax.named_scope(f"w_fin{p}"):
            fins[p].wait_recv()
        c = remote(piece(1 - x, p), piece(1 - x, p), s_frl, r_frl, d_mate)
        c.start()
        frels.append(c)
    with jax.named_scope("w_last"):
        last.wait_recv()
    write_lse(sq_own, sq_other)
    drain(aux.at[pl.ds(0, 3)], r_aux)
    for b in range(blocks):
        for h in range(n_comp // LANES):
            at = (b % 2) * n_comp + h * LANES
            lp_out[b // 2:b // 2 + 1, at:at + LANES] = aux[b, h:h + 1, :]
    with jax.named_scope("w_frel"):
        to_mate.wait_recv()
        drain(ssum, r_frl)
    with jax.named_scope("w_sends"):
        for c in (own, to_mate, last, counts):
            c.wait_send()
        drain(stats0.at[:, pl.ds(0, 2)], s_st0)
        drain(part.at[pl.ds(0, 2)], s_part)
        drain(xsend, s_xs)
        drain(xo, s_x)
        drain(xo, s_rel)
        drain(ssum, s_fin)
        drain(ssum, s_frl)
        drain(aux.at[pl.ds(0, 3)], s_aux)
        drain(stats.at[:, pl.ds(0, 3)], s_st)


def store_kernel(a, b, c, a_out, b_out, c_out, sem):
    copies = [
        pltpu.make_async_copy(src, dst, sem.at[i])
        for i, (src, dst) in enumerate(((a, a_out), (b, b_out), (c, c_out)))
    ]
    for c in copies:
        c.start()
    for c in copies:
        c.wait()


def solution(mesh):
    rows_size = mesh.shape["row"]
    comp_size = mesh.shape["comp"]

    def local_fit(x_local, mu_init, logpi_init, inv_temp):
        n_rows = x_local.shape[0]
        half = x_local.shape[1] // 2
        n_half = mu_init.shape[1]
        n_comp = n_half // 2
        sweeps = inv_temp.shape[0]
        total_pts = n_rows * rows_size
        n_tiles = total_pts // TILE
        tiles = n_rows // TILE
        halves = TILE // LANES
        vmem = pl.BlockSpec(memory_space=pltpu.VMEM)
        hbm = pl.BlockSpec(memory_space=pl.ANY)
        dma = pltpu.SemaphoreType.DMA
        outs = pl.pallas_call(
            functools.partial(em_kernel, sweeps, total_pts, n_half * comp_size),
            out_shape=(
                pltpu.VMEM(mu_init.shape, F32),
                pltpu.VMEM(logpi_init.shape, F32),
                pltpu.VMEM((2, n_rows), F32),
            ),
            in_specs=[hbm] * 4,
            out_specs=(vmem, vmem, vmem),
            scratch_shapes=[
                pltpu.SMEM((sweeps,), F32),
                pltpu.VMEM((n_rows, half), BF16),
                pltpu.VMEM((total_pts, half), BF16),
                pltpu.VMEM(mu_init.shape, F32),
                pltpu.VMEM(logpi_init.shape, F32),
                pltpu.VMEM((4, n_comp, half), BF16),
                pltpu.VMEM((4, n_comp, LANES), F32),
                pltpu.VMEM((2, 4, tiles, halves, LANES), F32),
                pltpu.VMEM((4, 2, n_comp, LANES), F32),
                pltpu.VMEM((2, 2, n_comp, LANES), F32),
                pltpu.VMEM((n_comp, half), F32),
                pltpu.VMEM((n_comp, half), F32),
                pltpu.VMEM((n_comp // LANES, LANES), F32),
                pltpu.VMEM((n_comp // LANES, LANES), F32),
                pltpu.VMEM((n_comp, half), BF16),
                pltpu.VMEM((n_comp, LANES), F32),
                pltpu.VMEM((n_tiles, n_comp, TILE), F32),
                pltpu.VMEM((n_tiles, halves, LANES), F32),
                pltpu.VMEM((sweeps - 1, 4, n_tiles, halves, LANES), F32),
                pltpu.VMEM((rows_size, n_comp, n_rows), BF16),
                pltpu.VMEM((n_comp, half), F32),
                pltpu.VMEM((n_comp, LANES), F32),
                pltpu.VMEM((n_tiles, halves, LANES), F32),
                pltpu.VMEM((tiles, halves, LANES), F32),
                pltpu.VMEM((rows_size, n_comp // LANES, LANES), F32),
                dma((5,)), dma, dma, dma, dma((tiles,)), dma, dma((tiles,)), dma, dma((2,)), dma, dma((2, 2)),
                dma, dma, dma, dma, dma, dma((sweeps - 1, rows_size)), dma, dma,
                dma, dma((PIECES,)), dma, dma, dma, dma, dma, dma,
            ],
            compiler_params=pltpu.CompilerParams(collective_id=0, has_side_effects=True),
        )(inv_temp, x_local, mu_init, logpi_init)
        outs = [pltpu.with_memory_space_constraint(o, pltpu.VMEM) for o in outs]
        return pl.pallas_call(
            store_kernel,
            out_shape=tuple(jax.ShapeDtypeStruct(o.shape, F32) for o in outs),
            in_specs=[vmem] * 3,
            out_specs=(hbm, hbm, hbm),
            scratch_shapes=[dma((3,))],
        )(*outs)

    return jax.shard_map(
        local_fit,
        mesh=mesh,
        in_specs=(P(("grp", "row"), None), P(None, ("grp", "comp"), None), P(None, ("grp", "comp")), P()),
        out_specs=(P(None, ("grp", "comp"), None), P(None, ("grp", "comp")), P(None, ("grp", "row"))),
        check_vma=False,
    )
```

```python
import functools

import jax
import jax.numpy as jnp
from jax import lax
from jax.experimental import pallas as pl
from jax.experimental.pallas import tpu as pltpu
from jax.sharding import PartitionSpec as P

EPS_COUNT = 1e-6
PRIOR_ALPHA = 1e-3
LOG2E = 1.4426950408889634
LN2 = 0.6931471805599453
LANES = 128
TILE = 256
FIRST = 8
EARLY = 4
PIECES = 4
CROSSINGS = ((0, 7), (7, 7), (14, 2))

MESH = pl.DeviceIdType.MESH
F32 = jnp.float32
BF16 = jnp.bfloat16
NT = (((1,), (1,)), ((), ()))


def em_kernel(
    sweeps, total_pts, total_comp,
    temp_in, x_in, mu_in, lp_in,
    mu_out, lp_out, lse_out,
    temp_ref, xo, xg, mu0, lp0, mub0, cc0, stats0, part, inbox, xsend, xin, nsend, nin,
    mub, cc, ee, mm, stats, rr, ssum, nacc, lse2, lse_in, aux,
    s_in, s_own, r_own, s_x, r_x, s_rel, r_rel, s_st0, r_st0, s_part, r_part, s_xs, r_xs, s_n, r_n,
    s_st, r_st, s_lse, r_lse, s_fin, r_fin, s_mate, r_mate, s_frl, r_frl, s_aux, r_aux,
):
    row = lax.axis_index("row")
    y = lax.axis_index("comp")
    x = row // 2
    core = row % 2
    me = 2 * y + core
    mate = 2 * x + 1 - core
    across = 2 * (1 - x) + core
    across_mate = 2 * (1 - x) + 1 - core
    across_one = 2 * (1 - x) + 1

    n_rows = xo.shape[0]
    n_comp = mub.shape[0]
    blocks = xg.shape[0] // n_rows
    tiles = n_rows // TILE
    halves = TILE // LANES
    fit_col = pl.ds(pl.multiple_of(x * LANES, LANES), LANES)
    other_col = pl.ds(pl.multiple_of((1 - x) * LANES, LANES), LANES)
    my_comps = pl.ds(pl.multiple_of(core * n_comp, n_comp), n_comp)
    mates_comps = pl.ds(pl.multiple_of((1 - core) * n_comp, n_comp), n_comp)
    my_rows = pl.ds(pl.multiple_of(row * n_rows, n_rows), n_rows)

    d_mate = {"row": mate}
    d_across = {"row": across}
    d_across_mate = {"row": across_mate}
    d_across_one = {"row": across_one}
    d_y = {"comp": 1 - y}
    d_y_mate = {"comp": 1 - y, "row": mate}

    def drain(ref, sem):
        pltpu.make_async_copy(ref, ref, sem).wait()

    def remote(src, dst, ssem, rsem, dev):
        return pltpu.make_async_remote_copy(src, dst, ssem, rsem, device_id=dev, device_id_type=MESH)

    loads = [
        pltpu.make_async_copy(src, dst, s_in.at[i])
        for i, (src, dst) in enumerate((
            (x_in.at[:, other_col], xo),
            (mu_in.at[1 - x], mu0.at[1 - x]),
            (lp_in, lp0),
            (temp_in, temp_ref),
            (x_in.at[:, fit_col], xg.at[my_rows, :]),
            (mu_in.at[x], mu0.at[x]),
        ))
    ]
    barrier = pltpu.get_barrier_semaphore()
    for dev in (d_mate, d_across, d_across_mate, d_y, d_y_mate):
        pl.semaphore_signal(barrier, inc=1, device_id=dev, device_id_type=MESH)
    for c in loads[:4]:
        c.start()
    with jax.named_scope("barrier"):
        pl.semaphore_wait(barrier, 5)
    for c in loads[4:]:
        c.start()
    with jax.named_scope("loads"):
        for c in loads[:4]:
            c.wait()

    def rows_of(block, j):
        return pl.ds(pl.multiple_of(block * n_rows + j * TILE, TILE), TILE)

    unit = n_rows // 16

    def some_rows(block, p):
        first, count = CROSSINGS[p]
        return pl.ds(pl.multiple_of(block * n_rows + first * unit, unit), count * unit)

    xs, relays = [], []
    for p, (first, count) in enumerate(CROSSINGS):
        xs.append(remote(xo.at[pl.ds(first * unit, count * unit), :], xg.at[some_rows(row, p), :],
                         s_x, r_x.at[p], d_across))
        got = xg.at[some_rows(across, p), :]
        relays.append(remote(got, got, s_rel, r_rel, d_mate))
    own = remote(xg.at[my_rows, :], xg.at[my_rows, :], s_own, r_own, d_mate)
    for c in xs[:-1]:
        c.start()

    def means_to(sweep, mean, logw, mub_at, cc_at):
        mub_at[...] = mean.astype(BF16)
        sq = jnp.sum(mean * mean, axis=1, keepdims=True)
        cc_at[...] = jnp.broadcast_to(LOG2E * (logw - temp_ref[sweep] * sq), cc_at.shape)

    def column(flat):
        return jnp.transpose(jnp.broadcast_to(flat, (LANES, n_comp)))

    def e_tile(sweep, t, a, cc_at, stat):
        scale = (2.0 * LOG2E) * temp_ref[sweep]
        for h in range(halves):
            z = a[:, h * LANES:(h + 1) * LANES] * scale + cc_at[...]
            m = jnp.max(z, axis=0, keepdims=True)
            e = jnp.exp2(z - m)
            r = jnp.sum(e, axis=0, keepdims=True)
            ee[t, :, h * LANES:(h + 1) * LANES] = e
            mm[t, h:h + 1, :] = m
            stat[h:h + 1, :] = m + jnp.log2(r)

    def lse_of(parts):
        top = jnp.maximum(jnp.maximum(parts[0], parts[1]), jnp.maximum(parts[2], parts[3]))
        tot = (jnp.exp2(parts[0] - top) + jnp.exp2(parts[1] - top)) + (
            jnp.exp2(parts[2] - top) + jnp.exp2(parts[3] - top))
        return top + jnp.log2(tot)

    def m_region(lses, base, pts, at, n_at, s_at, first):
        ws = []
        for j, lse in enumerate(lses):
            w = jnp.exp2(mm[base + j] - lse)
            ws += [w[h:h + 1, :] for h in range(halves)]
        for k in range(0, n_comp, 16):
            acc = None if first else n_at[k:k + 16, :]
            for v, w in enumerate(ws):
                r = ee[base + v // halves, k:k + 16, (v % halves) * LANES:(v % halves + 1) * LANES] * w
                acc = r if acc is None else acc + r
                rr[k:k + 16, at + v * LANES:at + (v + 1) * LANES] = r.astype(BF16)
            n_at[k:k + 16, :] = acc
        s = jnp.dot(rr[:, at:at + len(lses) * TILE], pts, preferred_element_type=F32)
        if first:
            s_at[...] = s
        else:
            s_at[...] += s

    def cross0(slot, j):
        pts = xg[rows_of(row, j), :] if slot // 2 else xo[pl.ds(j * TILE, TILE), :]
        return lax.dot_general(mub0[slot], pts, NT, preferred_element_type=F32)

    def st0_copy(fo):
        at = stats0.at[fo, pl.ds(2 * y, 2)]
        return remote(at, at, s_st0, r_st0.at[fo], d_y)

    for fo, fit in enumerate((1 - x, x)):
        with jax.named_scope(f"set0_{fo}"):
            for qo, comps in enumerate((mates_comps, my_comps)):
                slot = 2 * fo + qo
                means_to(0, mu0[fit, comps, :], column(lp0[pl.ds(fit, 1), comps]), mub0.at[slot], cc0.at[slot])
        with jax.named_scope(f"e0_{fo}"):
            order = [(2 * fo + qo, j) for qo in range(2) for j in range(tiles)]
            ahead = cross0(*order[0])
            for i, (slot, j) in enumerate(order):
                a = ahead
                if i + 1 < len(order):
                    ahead = cross0(*order[i + 1])
                e_tile(0, slot * tiles + j, a, cc0.at[slot], stats0.at[fo, 2 * y + slot % 2, j])
        st0_copy(fo).start()
        if fo == 0:
            for c in loads[4:]:
                c.wait()
            own.start()

    def part_copy(fo, k):
        return remote(part.at[2 * fo, k], inbox.at[fo, k], s_part, r_part.at[2 if fo else k], d_mate)

    def m0(fo, qo):
        slot = 2 * fo + qo
        lses = [lse_of([stats0[fo, d, j] for d in range(4)]) for j in range(tiles)]
        pts = xg[my_rows, :] if fo else xo[...]
        m_region(lses, slot * tiles, pts, slot * n_rows, part.at[slot, 1], part.at[slot, 0], True)

    step = n_comp // PIECES
    with jax.named_scope("w_st0_0"):
        st0_copy(0).wait_recv()
    with jax.named_scope("m0_0"):
        m0(0, 0)
    for k in range(2):
        part_copy(0, k).start()
    with jax.named_scope("m0_1"):
        m0(0, 1)
    with jax.named_scope("w_part0"):
        part_copy(0, 0).wait_recv()
    sums = []
    for p in range(PIECES):
        at = pl.ds(p * step, step)
        xsend[at, :] = (part[1, 0, at, :] + inbox[0, 0, at, :]).astype(BF16)
        c = remote(xsend.at[at, :], xin.at[at, :], s_xs, r_xs, d_across)
        c.start()
        sums.append(c)
    part_copy(0, 1).wait_recv()
    flat = jnp.sum(jnp.transpose(part[1, 1] + inbox[0, 1]), axis=0, keepdims=True)
    for h in range(n_comp // LANES):
        nsend[h:h + 1, :] = flat[:, h * LANES:(h + 1) * LANES]
    counts = remote(nsend, nin, s_n, r_n, d_across)
    counts.start()
    xs[-1].start()
    with jax.named_scope("w_st0_1"):
        st0_copy(1).wait_recv()
    with jax.named_scope("m0_2"):
        m0(1, 0)
    for k in range(2):
        part_copy(1, k).start()
    with jax.named_scope("m0_3"):
        m0(1, 1)
    for p in range(len(xs) - 1):
        with jax.named_scope(f"w_x{p}"):
            xs[p].wait_recv()
        relays[p].start()
    with jax.named_scope("w_part1"):
        drain(inbox.at[1], r_part.at[2])
    with jax.named_scope("w_xin"):
        counts.wait_recv()
        drain(xsend, r_xs)
    n_across = column(jnp.concatenate([nin[h:h + 1, :] for h in range(n_comp // LANES)], axis=1))
    ssum[...] = part[3, 0] + inbox[1, 0] + xin[...].astype(F32)
    n_first = jnp.sum(part[3, 1] + inbox[1, 1], axis=1, keepdims=True) + n_across

    def cross(t):
        return lax.dot_general(mub[...], xg[pl.ds(pl.multiple_of(t * TILE, TILE), TILE), :], NT,
                               preferred_element_type=F32)

    def st_send(sweep, group):
        t, count, sem = group
        at = stats.at[sweep - 1, me, pl.ds(t, count)]
        for dev in (d_y, d_y_mate, d_mate):
            remote(at, at, s_st, r_st.at[sweep - 1, sem], dev).start()

    def e_group(sweep, group):
        t, count, _ = group
        ahead = cross(t)
        for i in range(count):
            a = ahead
            if i + 1 < count:
                ahead = cross(t + i + 1)
            e_tile(sweep, t + i, a, cc, stats.at[sweep - 1, me, t + i])
        st_send(sweep, group)

    def m_group(sweep, t, count, sems, at, first):
        with jax.named_scope("stwait"):
            for sem in sems:
                drain(stats.at[sweep - 1, pl.ds(0, 3), pl.ds(0, count // len(sems))], r_st.at[sweep - 1, sem])
        with jax.named_scope("mgroup"):
            lses = []
            for j in range(count):
                lses.append(lse_of([stats[sweep - 1, d, t + j] for d in range(4)]))
                lse2[t + j] = lses[-1]
            pts = xg[pl.ds(pl.multiple_of(t * TILE, TILE), count * TILE), :]
            m_region(lses, t, pts, at, nacc, ssum, first)

    def finish(n):
        mean = ssum[...] / (n + EPS_COUNT)
        logw = jnp.log((n + PRIOR_ALPHA) / (total_pts + total_comp * PRIOR_ALPHA))
        return mean, logw

    with jax.named_scope("finish"):
        mean, logw = finish(n_first)
        means_to(1, mean, logw, mub, cc)
    for sweep in range(1, sweeps):
        if sweep == 1:
            near, far = 2 * x * tiles, 2 * (1 - x) * tiles
            with jax.named_scope("w_own"):
                own.wait_recv()
            with jax.named_scope("e_row_mate"):
                e_group(1, (near, EARLY, 0))
            with jax.named_scope("w_x3"):
                xs[-1].wait_recv()
            relays[-1].start()
            if EARLY < 2 * tiles:
                with jax.named_scope("e_row_mate2"):
                    e_group(1, (near + EARLY, 2 * tiles - EARLY, 3))
            with jax.named_scope("e_across"):
                e_group(1, (across * tiles, tiles, 1 + core))
            with jax.named_scope("w_rel"):
                drain(xo, r_rel)
            with jax.named_scope("e_across_mate"):
                e_group(1, (across_mate * tiles, tiles, 2 - core))
            m_group(1, near, 2 * tiles, (0, 3) if EARLY < 2 * tiles else (0,), 0, True)
            m_group(1, far, 2 * tiles, (1, 2), 2 * n_rows, False)
        else:
            n_tiles = blocks * tiles
            with jax.named_scope("esweep"):
                e_group(sweep, (0, FIRST, 0))
                e_group(sweep, (FIRST, n_tiles - FIRST, 1))
            m_group(sweep, 0, FIRST, (0,), 0, True)
            m_group(sweep, FIRST, n_tiles - FIRST, (1,), FIRST * TILE, False)
        with jax.named_scope("finish"):
            mean, logw = finish(jnp.sum(nacc[...], axis=1, keepdims=True))
            if sweep + 1 < sweeps:
                means_to(sweep + 1, mean, logw, mub, cc)

    mu_out[x, my_comps, :] = mean

    def piece(fit, one, p):
        return mu_out.at[fit, pl.ds(pl.multiple_of(one * n_comp + p * step, step), step), :]

    for p in range(PIECES):
        remote(piece(x, core, p), piece(x, core, p), s_fin, r_fin.at[core, p], d_across_one).start()
    whole = mu_out.at[x, my_comps, :]
    to_mate = remote(whole, whole, s_mate, r_mate, d_mate)
    to_mate.start()
    last = remote(lse2.at[pl.ds(across * tiles, tiles)], lse_in, s_lse, r_lse, d_across)
    last.start()
    flat = jnp.transpose(jnp.broadcast_to(logw, (n_comp, LANES)))[0:1, :]
    for h in range(n_comp // LANES):
        aux[row, h:h + 1, :] = flat[:, h * LANES:(h + 1) * LANES]
    auxs = []
    for k, dev in enumerate((d_mate, d_across, d_across_mate)):
        c = remote(aux.at[row], aux.at[row], s_aux, r_aux, dev)
        c.start()
        auxs.append(c)

    ones = jnp.ones((8, LANES), BF16)

    def sq_rows(pts):
        xf = pts.astype(F32)
        xx = xf * xf
        hi = xx.astype(BF16)
        lo = (xx - hi.astype(F32)).astype(BF16)
        sq = lax.dot_general(ones, hi, NT, preferred_element_type=F32)
        return sq + lax.dot_general(ones, lo, NT, preferred_element_type=F32)

    def write_lse(sq_own, sq_other):
        for s in range(2):
            sq = jnp.where(x == s, sq_own, sq_other)
            for j in range(tiles):
                val = jnp.where(x == s, lse2[row * tiles + j], lse_in[j])
                for h in range(halves):
                    at = slice(j * TILE + h * LANES, j * TILE + (h + 1) * LANES)
                    lse_out[s:s + 1, at] = val[h:h + 1, :] * LN2 - temp_ref[sweeps - 1] * sq[0:1, at]

    with jax.named_scope("lse"):
        sq_own = sq_rows(xg[my_rows, :])
        sq_other = sq_rows(xo[...])
    @pl.when(core == 1)
    def _():
        for p in range(PIECES):
            for one in (1, 0):
                got = piece(1 - x, one, p)
                with jax.named_scope(f"w_fin{p}{one}"):
                    remote(got, got, s_fin, r_fin.at[one, p], d_across).wait_recv()
                remote(got, got, s_frl, r_frl, d_mate).start()

    with jax.named_scope("w_last"):
        last.wait_recv()
    write_lse(sq_own, sq_other)
    drain(aux.at[pl.ds(0, 3)], r_aux)
    for b in range(blocks):
        for h in range(n_comp // LANES):
            at = (b % 2) * n_comp + h * LANES
            lp_out[b // 2:b // 2 + 1, at:at + LANES] = aux[b, h:h + 1, :]
    with jax.named_scope("w_frel"):
        to_mate.wait_recv()

        @pl.when(core == 0)
        def _():
            drain(mu_out.at[0], r_frl)

    with jax.named_scope("w_sends"):
        for c in (own, to_mate, last, counts):
            c.wait_send()
        drain(stats0.at[:, pl.ds(0, 2)], s_st0)
        drain(part.at[pl.ds(0, 2)], s_part)
        drain(xsend, s_xs)
        drain(xo, s_x)
        drain(xo, s_rel)
        drain(ssum, s_fin)

        @pl.when(core == 1)
        def _():
            drain(mu_out.at[0], s_frl)

        drain(aux.at[pl.ds(0, 3)], s_aux)
        drain(stats.at[:, pl.ds(0, 3)], s_st)


def store_kernel(a, b, c, a_out, b_out, c_out, sem):
    copies = [
        pltpu.make_async_copy(src, dst, sem.at[i])
        for i, (src, dst) in enumerate(((a, a_out), (b, b_out), (c, c_out)))
    ]
    for c in copies:
        c.start()
    for c in copies:
        c.wait()


def solution(mesh):
    rows_size = mesh.shape["row"]
    comp_size = mesh.shape["comp"]

    def local_fit(x_local, mu_init, logpi_init, inv_temp):
        n_rows = x_local.shape[0]
        half = x_local.shape[1] // 2
        n_half = mu_init.shape[1]
        n_comp = n_half // 2
        sweeps = inv_temp.shape[0]
        total_pts = n_rows * rows_size
        n_tiles = total_pts // TILE
        tiles = n_rows // TILE
        halves = TILE // LANES
        vmem = pl.BlockSpec(memory_space=pltpu.VMEM)
        hbm = pl.BlockSpec(memory_space=pl.ANY)
        dma = pltpu.SemaphoreType.DMA
        outs = pl.pallas_call(
            functools.partial(em_kernel, sweeps, total_pts, n_half * comp_size),
            out_shape=(
                pltpu.VMEM(mu_init.shape, F32),
                pltpu.VMEM(logpi_init.shape, F32),
                pltpu.VMEM((2, n_rows), F32),
            ),
            in_specs=[hbm] * 4,
            out_specs=(vmem, vmem, vmem),
            scratch_shapes=[
                pltpu.SMEM((sweeps,), F32),
                pltpu.VMEM((n_rows, half), BF16),
                pltpu.VMEM((total_pts, half), BF16),
                pltpu.VMEM(mu_init.shape, F32),
                pltpu.VMEM(logpi_init.shape, F32),
                pltpu.VMEM((4, n_comp, half), BF16),
                pltpu.VMEM((4, n_comp, LANES), F32),
                pltpu.VMEM((2, 4, tiles, halves, LANES), F32),
                pltpu.VMEM((4, 2, n_comp, LANES), F32),
                pltpu.VMEM((2, 2, n_comp, LANES), F32),
                pltpu.VMEM((n_comp, half), BF16),
                pltpu.VMEM((n_comp, half), BF16),
                pltpu.VMEM((n_comp // LANES, LANES), F32),
                pltpu.VMEM((n_comp // LANES, LANES), F32),
                pltpu.VMEM((n_comp, half), BF16),
                pltpu.VMEM((n_comp, LANES), F32),
                pltpu.VMEM((n_tiles, n_comp, TILE), F32),
                pltpu.VMEM((n_tiles, halves, LANES), F32),
                pltpu.VMEM((sweeps - 1, 4, n_tiles, halves, LANES), F32),
                pltpu.VMEM((n_comp, total_pts), BF16),
                pltpu.VMEM((n_comp, half), F32),
                pltpu.VMEM((n_comp, LANES), F32),
                pltpu.VMEM((n_tiles, halves, LANES), F32),
                pltpu.VMEM((tiles, halves, LANES), F32),
                pltpu.VMEM((rows_size, n_comp // LANES, LANES), F32),
                dma((6,)), dma, dma, dma, dma((len(CROSSINGS),)), dma, dma, dma, dma((2,)), dma, dma((3,)),
                dma, dma, dma, dma, dma, dma((sweeps - 1, 4)), dma, dma,
                dma, dma((2, PIECES)), dma, dma, dma, dma, dma, dma,
            ],
            compiler_params=pltpu.CompilerParams(collective_id=0, has_side_effects=True),
        )(inv_temp, x_local, mu_init, logpi_init)
        outs = [pltpu.with_memory_space_constraint(o, pltpu.VMEM) for o in outs]
        return pl.pallas_call(
            store_kernel,
            out_shape=tuple(jax.ShapeDtypeStruct(o.shape, F32) for o in outs),
            in_specs=[vmem] * 3,
            out_specs=(hbm, hbm, hbm),
            scratch_shapes=[dma((3,))],
        )(*outs)

    return jax.shard_map(
        local_fit,
        mesh=mesh,
        in_specs=(P(("grp", "row"), None), P(None, ("grp", "comp"), None), P(None, ("grp", "comp")), P()),
        out_specs=(P(None, ("grp", "comp"), None), P(None, ("grp", "comp")), P(None, ("grp", "row"))),
        check_vma=False,
    )
```

```python
import functools

import jax
import jax.numpy as jnp
from jax import lax
from jax.experimental import pallas as pl
from jax.experimental.pallas import tpu as pltpu
from jax.sharding import PartitionSpec as P

EPS_COUNT = 1e-6
PRIOR_ALPHA = 1e-3
LOG2E = 1.4426950408889634
LN2 = 0.6931471805599453
LANES = 128
TILE = 256
FIRST = 8
EARLY = 4
PIECES = 4
CROSSINGS = ((0, 7), (7, 8), (15, 1))

MESH = pl.DeviceIdType.MESH
F32 = jnp.float32
BF16 = jnp.bfloat16
NT = (((1,), (1,)), ((), ()))


def em_kernel(
    sweeps, total_pts, total_comp,
    temp_in, x_in, mu_in, lp_in,
    mu_out, lp_out, lse_out,
    temp_ref, xo, xg, mu0, lp0, mub0, cc0, stats0, part, inbox, xsend, xin, nsend, nin,
    mub, cc, ee, mm, stats, rr, ssum, nacc, lse2, lse_in, aux,
    s_in, s_out, r_own, r_x, r_rel, r_st0, r_part, r_xs, r_n, r_st, r_lse, r_fin, r_mate, r_frl, r_aux,
):
    row = lax.axis_index("row")
    y = lax.axis_index("comp")
    x = row // 2
    core = row % 2
    me = 2 * y + core
    mate = 2 * x + 1 - core
    across = 2 * (1 - x) + core
    across_mate = 2 * (1 - x) + 1 - core
    across_one = 2 * (1 - x) + 1

    n_rows = xo.shape[0]
    n_comp = mub.shape[0]
    blocks = xg.shape[0] // n_rows
    tiles = n_rows // TILE
    halves = TILE // LANES
    fit_col = pl.ds(pl.multiple_of(x * LANES, LANES), LANES)
    other_col = pl.ds(pl.multiple_of((1 - x) * LANES, LANES), LANES)
    my_comps = pl.ds(pl.multiple_of(core * n_comp, n_comp), n_comp)
    mates_comps = pl.ds(pl.multiple_of((1 - core) * n_comp, n_comp), n_comp)
    my_rows = pl.ds(pl.multiple_of(row * n_rows, n_rows), n_rows)

    d_mate = {"row": mate}
    d_across = {"row": across}
    d_across_mate = {"row": across_mate}
    d_across_one = {"row": across_one}
    d_y = {"comp": 1 - y}
    d_y_mate = {"comp": 1 - y, "row": mate}

    def drain(ref, sem):
        pltpu.make_async_copy(ref, ref, sem).wait()

    def remote(src, dst, ssem, rsem, dev):
        return pltpu.make_async_remote_copy(src, dst, ssem, rsem, device_id=dev, device_id_type=MESH)

    loads = [
        pltpu.make_async_copy(src, dst, s_in.at[i])
        for i, (src, dst) in enumerate((
            (x_in.at[:, other_col], xo),
            (mu_in.at[1 - x], mu0.at[1 - x]),
            (lp_in, lp0),
            (temp_in, temp_ref),
            (x_in.at[:, fit_col], xg.at[my_rows, :]),
            (mu_in.at[x], mu0.at[x]),
        ))
    ]
    barrier = pltpu.get_barrier_semaphore()
    for dev in (d_mate, d_across, d_across_mate, d_y, d_y_mate):
        pl.semaphore_signal(barrier, inc=1, device_id=dev, device_id_type=MESH)
    for c in loads[:4]:
        c.start()
    with jax.named_scope("barrier"):
        pl.semaphore_wait(barrier, 5)
    for c in loads[4:]:
        c.start()
    with jax.named_scope("loads"):
        loads[0].wait()

    def rows_of(block, j):
        return pl.ds(pl.multiple_of(block * n_rows + j * TILE, TILE), TILE)

    unit = n_rows // 16

    def some_rows(block, p):
        first, count = CROSSINGS[p]
        return pl.ds(pl.multiple_of(block * n_rows + first * unit, unit), count * unit)

    xs, relays = [], []
    for p, (first, count) in enumerate(CROSSINGS):
        xs.append(remote(xo.at[pl.ds(first * unit, count * unit), :], xg.at[some_rows(row, p), :],
                         s_out, r_x.at[p], d_across))
        got = xg.at[some_rows(across, p), :]
        relays.append(remote(got, got, s_out, r_rel.at[int(p == len(CROSSINGS) - 1)], d_mate))
    own = remote(xg.at[my_rows, :], xg.at[my_rows, :], s_out, r_own, d_mate)
    for c in xs[:-1]:
        c.start()
    for c in loads[1:4]:
        c.wait()

    def means_to(sweep, mean, logw, mub_at, cc_at):
        mub_at[...] = mean.astype(BF16)
        sq = jnp.sum(mean * mean, axis=1, keepdims=True)
        cc_at[...] = jnp.broadcast_to(LOG2E * (logw - temp_ref[sweep] * sq), cc_at.shape)

    def column(flat):
        return jnp.transpose(jnp.broadcast_to(flat, (LANES, n_comp)))

    def e_tile(sweep, t, a, cc_at, stat):
        scale = (2.0 * LOG2E) * temp_ref[sweep]
        for h in range(halves):
            z = a[:, h * LANES:(h + 1) * LANES] * scale + cc_at[...]
            m = jnp.max(z, axis=0, keepdims=True)
            e = jnp.exp2(z - m)
            r = jnp.sum(e, axis=0, keepdims=True)
            ee[t, :, h * LANES:(h + 1) * LANES] = e
            mm[t, h:h + 1, :] = m
            stat[h:h + 1, :] = m + jnp.log2(r)

    def lse_of(parts):
        top = jnp.maximum(jnp.maximum(parts[0], parts[1]), jnp.maximum(parts[2], parts[3]))
        tot = (jnp.exp2(parts[0] - top) + jnp.exp2(parts[1] - top)) + (
            jnp.exp2(parts[2] - top) + jnp.exp2(parts[3] - top))
        return top + jnp.log2(tot)

    def m_region(lses, base, pts, at, n_at, s_at, first, lo=0, hi=n_comp):
        ws = []
        for j, lse in enumerate(lses):
            w = jnp.exp2(mm[base + j] - lse)
            ws += [w[h:h + 1, :] for h in range(halves)]
        for k in range(lo, hi, 16):
            acc = None if first else n_at[k:k + 16, :]
            for v, w in enumerate(ws):
                r = ee[base + v // halves, k:k + 16, (v % halves) * LANES:(v % halves + 1) * LANES] * w
                acc = r if acc is None else acc + r
                rr[k:k + 16, at + v * LANES:at + (v + 1) * LANES] = r.astype(BF16)
            n_at[k:k + 16, :] = acc
        s = jnp.dot(rr[lo:hi, at:at + len(lses) * TILE], pts, preferred_element_type=F32)
        if first:
            s_at[lo:hi, :] = s
        else:
            s_at[lo:hi, :] += s

    def cross0(slot, j):
        pts = xg[rows_of(row, j), :] if slot // 2 else xo[pl.ds(j * TILE, TILE), :]
        return lax.dot_general(mub0[slot], pts, NT, preferred_element_type=F32)

    def st0_copy(fo):
        at = stats0.at[fo, pl.ds(2 * y, 2)]
        return remote(at, at, s_out, r_st0.at[fo], d_y)

    for fo, fit in enumerate((1 - x, x)):
        with jax.named_scope(f"set0_{fo}"):
            for qo, comps in enumerate((mates_comps, my_comps)):
                slot = 2 * fo + qo
                means_to(0, mu0[fit, comps, :], column(lp0[pl.ds(fit, 1), comps]), mub0.at[slot], cc0.at[slot])
        with jax.named_scope(f"e0_{fo}"):
            order = [(2 * fo + qo, j) for qo in range(2) for j in range(tiles)]
            ahead = cross0(*order[0])
            for i, (slot, j) in enumerate(order):
                a = ahead
                if i + 1 < len(order):
                    ahead = cross0(*order[i + 1])
                e_tile(0, slot * tiles + j, a, cc0.at[slot], stats0.at[fo, 2 * y + slot % 2, j])
        st0_copy(fo).start()
        if fo == 0:
            for c in loads[4:]:
                c.wait()
            own.start()

    def part_copy(fo, k):
        return remote(part.at[2 * fo, k], inbox.at[fo, k], s_out, r_part.at[2 if fo else k], d_mate)

    def m0(fo, qo):
        slot = 2 * fo + qo
        lses = [lse_of([stats0[fo, d, j] for d in range(4)]) for j in range(tiles)]
        pts = xg[my_rows, :] if fo else xo[...]
        m_region(lses, slot * tiles, pts, slot * n_rows, part.at[slot, 1], part.at[slot, 0], True)

    step = n_comp // PIECES
    with jax.named_scope("w_st0_0"):
        st0_copy(0).wait_recv()
    with jax.named_scope("m0_0"):
        m0(0, 0)
    for k in range(2):
        part_copy(0, k).start()
    with jax.named_scope("m0_1"):
        m0(0, 1)
    with jax.named_scope("w_part0"):
        part_copy(0, 0).wait_recv()
    sums = []
    for p in range(PIECES):
        at = pl.ds(p * step, step)
        xsend[at, :] = (part[1, 0, at, :] + inbox[0, 0, at, :]).astype(BF16)
        c = remote(xsend.at[at, :], xin.at[at, :], s_out, r_xs, d_across)
        c.start()
        sums.append(c)
    part_copy(0, 1).wait_recv()
    flat = jnp.sum(jnp.transpose(part[1, 1] + inbox[0, 1]), axis=0, keepdims=True)
    for h in range(n_comp // LANES):
        nsend[h:h + 1, :] = flat[:, h * LANES:(h + 1) * LANES]
    counts = remote(nsend, nin, s_out, r_n, d_across)
    counts.start()
    xs[-1].start()
    with jax.named_scope("w_st0_1"):
        st0_copy(1).wait_recv()
    with jax.named_scope("m0_2"):
        m0(1, 0)
    for k in range(2):
        part_copy(1, k).start()
    with jax.named_scope("m0_3"):
        m0(1, 1)
    for p in range(len(xs) - 1):
        with jax.named_scope(f"w_x{p}"):
            xs[p].wait_recv()
        relays[p].start()
    with jax.named_scope("w_part1"):
        drain(inbox.at[1], r_part.at[2])
    with jax.named_scope("w_xin"):
        counts.wait_recv()
        drain(xsend, r_xs)
    n_across = column(jnp.concatenate([nin[h:h + 1, :] for h in range(n_comp // LANES)], axis=1))
    ssum[...] = part[3, 0] + inbox[1, 0] + xin[...].astype(F32)
    n_first = jnp.sum(part[3, 1] + inbox[1, 1], axis=1, keepdims=True) + n_across

    def cross(t):
        return lax.dot_general(mub[...], xg[pl.ds(pl.multiple_of(t * TILE, TILE), TILE), :], NT,
                               preferred_element_type=F32)

    def st_send(sweep, group):
        t, count, sem = group[:3]
        at = stats.at[sweep - 1, me, pl.ds(t, count)]
        for dev in (d_y, d_y_mate, d_mate):
            remote(at, at, s_out, r_st.at[sweep - 1, sem], dev).start()

    def e_group(sweep, *groups):
        todo = [t + i for t, count, _ in groups for i in range(count)]
        ahead = cross(todo[0])
        for i, t in enumerate(todo):
            a = ahead
            if i + 1 < len(todo):
                ahead = cross(todo[i + 1])
            e_tile(sweep, t, a, cc, stats.at[sweep - 1, me, t])
        for group in groups:
            st_send(sweep, group)

    def m_group(sweep, t, count, sems, at, first, after=None):
        with jax.named_scope("stwait"):
            for sem in sems:
                drain(stats.at[sweep - 1, pl.ds(0, 3), pl.ds(0, count // len(sems))], r_st.at[sweep - 1, sem])
        with jax.named_scope("mgroup"):
            lses = []
            for j in range(count):
                lses.append(lse_of([stats[sweep - 1, d, t + j] for d in range(4)]))
                lse2[t + j] = lses[-1]
            pts = xg[pl.ds(pl.multiple_of(t * TILE, TILE), count * TILE), :]
            if after is None:
                m_region(lses, t, pts, at, nacc, ssum, first)
            else:
                for lo in range(0, n_comp, n_comp // 2):
                    m_region(lses, t, pts, at, nacc, ssum, first, lo, lo + n_comp // 2)
                    after(lo, lo + n_comp // 2)

    def finish(n):
        mean = ssum[...] / (n + EPS_COUNT)
        logw = jnp.log((n + PRIOR_ALPHA) / (total_pts + total_comp * PRIOR_ALPHA))
        return mean, logw

    def piece(fit, one, p):
        return mu_out.at[fit, pl.ds(pl.multiple_of(one * n_comp + p * step, step), step), :]

    def send_final(lo, hi):
        n = jnp.sum(nacc[lo:hi, :], axis=1, keepdims=True)
        mu_out[x, pl.ds(pl.multiple_of(core * n_comp + lo, step), hi - lo), :] = ssum[lo:hi, :] / (n + EPS_COUNT)
        for p in range(lo // step, hi // step):
            remote(piece(x, core, p), piece(x, core, p), s_out, r_fin.at[p], d_across_one).start()

    with jax.named_scope("finish"):
        mean, logw = finish(n_first)
        means_to(1, mean, logw, mub, cc)
    for sweep in range(1, sweeps):
        if sweep == 1:
            near, far = 2 * x * tiles, 2 * (1 - x) * tiles
            with jax.named_scope("w_own"):
                own.wait_recv()
            with jax.named_scope("e_row_mate"):
                e_group(1, (near, EARLY, 0))
            with jax.named_scope("w_x3"):
                xs[-1].wait_recv()
            relays[-1].start()
            if EARLY < 2 * tiles:
                with jax.named_scope("e_row_mate2"):
                    e_group(1, (near + EARLY, 2 * tiles - EARLY, 3))
            most = tiles - 1
            with jax.named_scope("w_rel"):
                drain(xg.at[pl.ds(0, (CROSSINGS[-1][0] * n_rows) // 16), :], r_rel.at[0])
            with jax.named_scope("e_far"):
                e_group(1, (across * tiles, most, 1), (across_mate * tiles, most, 1))
            with jax.named_scope("w_rel"):
                drain(xg.at[pl.ds(0, (CROSSINGS[-1][1] * n_rows) // 16), :], r_rel.at[1])
            with jax.named_scope("e_far2"):
                e_group(1, (across * tiles + most, 1, 1), (across_mate * tiles + most, 1, 1))
            m_group(1, near, 2 * tiles, (0, 3) if EARLY < 2 * tiles else (0,), 0, True)
            m_group(1, far, 2 * tiles, (1,), 2 * n_rows, False)
        else:
            n_tiles = blocks * tiles
            with jax.named_scope("esweep"):
                e_group(sweep, (0, FIRST, 0))
                e_group(sweep, (FIRST, n_tiles - FIRST, 1))
            m_group(sweep, 0, FIRST, (0,), 0, True)
            m_group(sweep, FIRST, n_tiles - FIRST, (1,), FIRST * TILE, False,
                    send_final if sweep == sweeps - 1 else None)
        if sweep < sweeps - 1:
            with jax.named_scope("finish"):
                mean, logw = finish(jnp.sum(nacc[...], axis=1, keepdims=True))
                means_to(sweep + 1, mean, logw, mub, cc)

    whole = mu_out.at[x, my_comps, :]
    to_mate = remote(whole, whole, s_out, r_mate, d_mate)
    to_mate.start()
    last = remote(lse2.at[pl.ds(across * tiles, tiles)], lse_in, s_out, r_lse, d_across)
    last.start()
    n_last = jnp.sum(jnp.transpose(nacc[...]), axis=0, keepdims=True)
    flat = jnp.log((n_last + PRIOR_ALPHA) / (total_pts + total_comp * PRIOR_ALPHA))
    for h in range(n_comp // LANES):
        aux[row, h:h + 1, :] = flat[:, h * LANES:(h + 1) * LANES]
    auxs = []
    for k, dev in enumerate((d_mate, d_across, d_across_mate)):
        c = remote(aux.at[row], aux.at[row], s_out, r_aux, dev)
        c.start()
        auxs.append(c)

    ones = jnp.ones((8, LANES), BF16)

    def sq_rows(pts):
        xf = pts.astype(F32)
        xx = xf * xf
        hi = xx.astype(BF16)
        lo = (xx - hi.astype(F32)).astype(BF16)
        sq = lax.dot_general(ones, hi, NT, preferred_element_type=F32)
        return sq + lax.dot_general(ones, lo, NT, preferred_element_type=F32)

    def write_lse(sq_own, sq_other):
        for s in range(2):
            sq = jnp.where(x == s, sq_own, sq_other)
            for j in range(tiles):
                val = jnp.where(x == s, lse2[row * tiles + j], lse_in[j])
                for h in range(halves):
                    at = slice(j * TILE + h * LANES, j * TILE + (h + 1) * LANES)
                    lse_out[s:s + 1, at] = val[h:h + 1, :] * LN2 - temp_ref[sweeps - 1] * sq[0:1, at]

    with jax.named_scope("lse"):
        sq_own = sq_rows(xg[my_rows, :])
        sq_other = sq_rows(xo[...])
    @pl.when(core == 1)
    def _():
        for p in range(PIECES):
            with jax.named_scope(f"w_fin{p}"):
                drain(ssum.at[pl.ds(0, 2 * step)], r_fin.at[p])
            for one in range(2):
                got = piece(1 - x, one, p)
                remote(got, got, s_out, r_frl, d_mate).start()

    with jax.named_scope("w_last"):
        last.wait_recv()
    write_lse(sq_own, sq_other)
    drain(aux.at[pl.ds(0, 3)], r_aux)
    for b in range(blocks):
        for h in range(n_comp // LANES):
            at = (b % 2) * n_comp + h * LANES
            lp_out[b // 2:b // 2 + 1, at:at + LANES] = aux[b, h:h + 1, :]
    with jax.named_scope("w_frel"):
        to_mate.wait_recv()

        @pl.when(core == 0)
        def _():
            drain(mu_out.at[0], r_frl)

    with jax.named_scope("w_sends"):
        for c in (own, to_mate, last, counts):
            c.wait_send()
        drain(stats0.at[:, pl.ds(0, 2)], s_out)
        drain(part.at[pl.ds(0, 2)], s_out)
        drain(xsend, s_out)
        drain(xo, s_out)
        drain(xo, s_out)
        drain(ssum, s_out)

        @pl.when(core == 1)
        def _():
            drain(mu_out.at[0], s_out)

        drain(aux.at[pl.ds(0, 3)], s_out)
        drain(stats.at[:, pl.ds(0, 3)], s_out)


def store_kernel(a, b, c, a_out, b_out, c_out, sem):
    copies = [
        pltpu.make_async_copy(src, dst, sem.at[i])
        for i, (src, dst) in enumerate(((a, a_out), (b, b_out), (c, c_out)))
    ]
    for c in copies:
        c.start()
    for c in copies:
        c.wait()


def solution(mesh):
    rows_size = mesh.shape["row"]
    comp_size = mesh.shape["comp"]

    def local_fit(x_local, mu_init, logpi_init, inv_temp):
        n_rows = x_local.shape[0]
        half = x_local.shape[1] // 2
        n_half = mu_init.shape[1]
        n_comp = n_half // 2
        sweeps = inv_temp.shape[0]
        total_pts = n_rows * rows_size
        n_tiles = total_pts // TILE
        tiles = n_rows // TILE
        halves = TILE // LANES
        vmem = pl.BlockSpec(memory_space=pltpu.VMEM)
        hbm = pl.BlockSpec(memory_space=pl.ANY)
        dma = pltpu.SemaphoreType.DMA
        outs = pl.pallas_call(
            functools.partial(em_kernel, sweeps, total_pts, n_half * comp_size),
            out_shape=(
                pltpu.VMEM(mu_init.shape, F32),
                pltpu.VMEM(logpi_init.shape, F32),
                pltpu.VMEM((2, n_rows), F32),
            ),
            in_specs=[hbm] * 4,
            out_specs=(vmem, vmem, vmem),
            scratch_shapes=[
                pltpu.SMEM((sweeps,), F32),
                pltpu.VMEM((n_rows, half), BF16),
                pltpu.VMEM((total_pts, half), BF16),
                pltpu.VMEM(mu_init.shape, F32),
                pltpu.VMEM(logpi_init.shape, F32),
                pltpu.VMEM((4, n_comp, half), BF16),
                pltpu.VMEM((4, n_comp, LANES), F32),
                pltpu.VMEM((2, 4, tiles, halves, LANES), F32),
                pltpu.VMEM((4, 2, n_comp, LANES), F32),
                pltpu.VMEM((2, 2, n_comp, LANES), F32),
                pltpu.VMEM((n_comp, half), BF16),
                pltpu.VMEM((n_comp, half), BF16),
                pltpu.VMEM((n_comp // LANES, LANES), F32),
                pltpu.VMEM((n_comp // LANES, LANES), F32),
                pltpu.VMEM((n_comp, half), BF16),
                pltpu.VMEM((n_comp, LANES), F32),
                pltpu.VMEM((n_tiles, n_comp, TILE), F32),
                pltpu.VMEM((n_tiles, halves, LANES), F32),
                pltpu.VMEM((sweeps - 1, 4, n_tiles, halves, LANES), F32),
                pltpu.VMEM((n_comp, total_pts), BF16),
                pltpu.VMEM((n_comp, half), F32),
                pltpu.VMEM((n_comp, LANES), F32),
                pltpu.VMEM((n_tiles, halves, LANES), F32),
                pltpu.VMEM((tiles, halves, LANES), F32),
                pltpu.VMEM((rows_size, n_comp // LANES, LANES), F32),
                dma((6,)), dma, dma, dma((len(CROSSINGS),)), dma((2,)), dma((2,)), dma((3,)), dma, dma,
                dma((sweeps - 1, 4)), dma, dma((PIECES,)), dma, dma, dma,
            ],
            compiler_params=pltpu.CompilerParams(collective_id=0, has_side_effects=True),
        )(inv_temp, x_local, mu_init, logpi_init)
        outs = [pltpu.with_memory_space_constraint(o, pltpu.VMEM) for o in outs]
        return pl.pallas_call(
            store_kernel,
            out_shape=tuple(jax.ShapeDtypeStruct(o.shape, F32) for o in outs),
            in_specs=[vmem] * 3,
            out_specs=(hbm, hbm, hbm),
            scratch_shapes=[dma((3,))],
        )(*outs)

    return jax.shard_map(
        local_fit,
        mesh=mesh,
        in_specs=(P(("grp", "row"), None), P(None, ("grp", "comp"), None), P(None, ("grp", "comp")), P()),
        out_specs=(P(None, ("grp", "comp"), None), P(None, ("grp", "comp")), P(None, ("grp", "row"))),
        check_vma=False,
    )
```

```python
import functools

import jax
import jax.numpy as jnp
from jax import lax
from jax.experimental import pallas as pl
from jax.experimental.pallas import tpu as pltpu
from jax.sharding import PartitionSpec as P

EPS_COUNT = 1e-6
PRIOR_ALPHA = 1e-3
LOG2E = 1.4426950408889634
LN2 = 0.6931471805599453
LANES = 128
TILE = 256
FIRST = 8
PIECES = 4
SHARED = 3

MESH = pl.DeviceIdType.MESH
F32 = jnp.float32
BF16 = jnp.bfloat16
NT = (((1,), (1,)), ((), ()))


def em_kernel(
    sweeps, total_pts, total_comp,
    temp_in, x_in, mu_in, lp_in,
    mu_out, lp_out, lse_out,
    temp_ref, xo, xg, mu0, lp0, mub0, cc0, stats0, part, inbox, xsend, xin, nsend, nin,
    mub, cc, ee, mm, stats, rr, ssum, nacc, lse2, lse_in, aux,
    s_in, s_out, r_own, r_x, r_y, r_rel, r_st0, r_part, r_xs, r_n, r_st, r_lse, r_fin, r_mate, r_frl, r_aux,
):
    row = lax.axis_index("row")
    y = lax.axis_index("comp")
    x = row // 2
    core = row % 2
    me = 2 * y + core
    mate = 2 * x + 1 - core
    across = 2 * (1 - x) + core
    across_mate = 2 * (1 - x) + 1 - core
    across_one = 2 * (1 - x) + 1

    n_rows = xo.shape[0]
    n_comp = mub.shape[0]
    blocks = xg.shape[0] // n_rows
    tiles = n_rows // TILE
    halves = TILE // LANES
    fit_col = pl.ds(pl.multiple_of(x * LANES, LANES), LANES)
    other_col = pl.ds(pl.multiple_of((1 - x) * LANES, LANES), LANES)
    my_comps = pl.ds(pl.multiple_of(core * n_comp, n_comp), n_comp)
    mates_comps = pl.ds(pl.multiple_of((1 - core) * n_comp, n_comp), n_comp)
    my_rows = pl.ds(pl.multiple_of(row * n_rows, n_rows), n_rows)

    d_mate = {"row": mate}
    d_across = {"row": across}
    d_across_mate = {"row": across_mate}
    d_across_one = {"row": across_one}
    d_y = {"comp": 1 - y}
    d_y_mate = {"comp": 1 - y, "row": mate}

    def drain(ref, sem):
        pltpu.make_async_copy(ref, ref, sem).wait()

    def remote(src, dst, ssem, rsem, dev):
        return pltpu.make_async_remote_copy(src, dst, ssem, rsem, device_id=dev, device_id_type=MESH)

    loads = [
        pltpu.make_async_copy(src, dst, s_in.at[i])
        for i, (src, dst) in enumerate((
            (x_in.at[:, other_col], xo),
            (mu_in.at[1 - x], mu0.at[1 - x]),
            (lp_in, lp0),
            (temp_in, temp_ref),
            (x_in.at[:, fit_col], xg.at[my_rows, :]),
            (mu_in.at[x], mu0.at[x]),
        ))
    ]
    barrier = pltpu.get_barrier_semaphore()
    for dev in (d_mate, d_across, d_across_mate, d_y, d_y_mate):
        pl.semaphore_signal(barrier, inc=1, device_id=dev, device_id_type=MESH)
    for c in loads[:4]:
        c.start()
    with jax.named_scope("barrier"):
        pl.semaphore_wait(barrier, 5)
    for c in loads[4:]:
        c.start()
    with jax.named_scope("loads"):
        loads[0].wait()

    def rows_of(block, j):
        return pl.ds(pl.multiple_of(block * n_rows + j * TILE, TILE), TILE)

    unit = n_rows // 16
    both = 16 - 2 * SHARED
    once = both + SHARED * y
    chunks = ((once, SHARED), (0, both // 2), (both // 2, both - both // 2))

    def some_rows(block, first, count):
        return pl.ds(pl.multiple_of(block * n_rows + first * unit, unit), count * unit)

    xs, relays = [], []
    for p, (first, count) in enumerate(chunks):
        xs.append(remote(xo.at[some_rows(0, first, count), :], xg.at[some_rows(row, first, count), :],
                         s_out, r_x.at[p], d_across))
        got = xg.at[some_rows(across, first, count), :]
        relays.append(remote(got, got, s_out, r_rel, d_mate))
    got = xg.at[some_rows(across, once, SHARED), :]
    over_y = remote(got, got, s_out, r_y, d_y)
    got = xg.at[some_rows(across, both + SHARED * (1 - y), SHARED), :]
    relays.append(remote(got, got, s_out, r_rel, d_mate))
    own = remote(xg.at[my_rows, :], xg.at[my_rows, :], s_out, r_own, d_mate)
    for c in xs:
        c.start()
    for c in loads[1:4]:
        c.wait()

    def means_to(sweep, mean, logw, mub_at, cc_at):
        mub_at[...] = mean.astype(BF16)
        sq = jnp.sum(mean * mean, axis=1, keepdims=True)
        cc_at[...] = jnp.broadcast_to(LOG2E * (logw - temp_ref[sweep] * sq), cc_at.shape)

    def column(flat):
        return jnp.transpose(jnp.broadcast_to(flat, (LANES, n_comp)))

    def e_tile(sweep, t, a, cc_at, stat):
        scale = (2.0 * LOG2E) * temp_ref[sweep]
        for h in range(halves):
            z = a[:, h * LANES:(h + 1) * LANES] * scale + cc_at[...]
            m = jnp.max(z, axis=0, keepdims=True)
            e = jnp.exp2(z - m)
            r = jnp.sum(e, axis=0, keepdims=True)
            ee[t, :, h * LANES:(h + 1) * LANES] = e
            mm[t, h:h + 1, :] = m
            stat[h:h + 1, :] = m + jnp.log2(r)

    def lse_of(parts):
        top = jnp.maximum(jnp.maximum(parts[0], parts[1]), jnp.maximum(parts[2], parts[3]))
        tot = (jnp.exp2(parts[0] - top) + jnp.exp2(parts[1] - top)) + (
            jnp.exp2(parts[2] - top) + jnp.exp2(parts[3] - top))
        return top + jnp.log2(tot)

    def m_region(lses, base, pts, at, n_at, s_at, first, lo=0, hi=n_comp):
        ws = []
        for j, lse in enumerate(lses):
            w = jnp.exp2(mm[base + j] - lse)
            ws += [w[h:h + 1, :] for h in range(halves)]
        for k in range(lo, hi, 16):
            acc = None if first else n_at[k:k + 16, :]
            for v, w in enumerate(ws):
                r = ee[base + v // halves, k:k + 16, (v % halves) * LANES:(v % halves + 1) * LANES] * w
                acc = r if acc is None else acc + r
                rr[k:k + 16, at + v * LANES:at + (v + 1) * LANES] = r.astype(BF16)
            n_at[k:k + 16, :] = acc
        s = jnp.dot(rr[lo:hi, at:at + len(lses) * TILE], pts, preferred_element_type=F32)
        if first:
            s_at[lo:hi, :] = s
        else:
            s_at[lo:hi, :] += s

    def cross0(slot, j):
        pts = xg[rows_of(row, j), :] if slot // 2 else xo[pl.ds(j * TILE, TILE), :]
        return lax.dot_general(mub0[slot], pts, NT, preferred_element_type=F32)

    def st0_copy(fo):
        at = stats0.at[fo, pl.ds(2 * y, 2)]
        return remote(at, at, s_out, r_st0.at[fo], d_y)

    for fo, fit in enumerate((1 - x, x)):
        with jax.named_scope(f"set0_{fo}"):
            for qo, comps in enumerate((mates_comps, my_comps)):
                slot = 2 * fo + qo
                means_to(0, mu0[fit, comps, :], column(lp0[pl.ds(fit, 1), comps]), mub0.at[slot], cc0.at[slot])
        with jax.named_scope(f"e0_{fo}"):
            order = [(2 * fo + qo, j) for qo in range(2) for j in range(tiles)]
            ahead = cross0(*order[0])
            for i, (slot, j) in enumerate(order):
                a = ahead
                if i + 1 < len(order):
                    ahead = cross0(*order[i + 1])
                e_tile(0, slot * tiles + j, a, cc0.at[slot], stats0.at[fo, 2 * y + slot % 2, j])
        st0_copy(fo).start()
        if fo == 0:
            for c in loads[4:]:
                c.wait()
            own.start()

    def part_copy(fo, k):
        return remote(part.at[2 * fo, k], inbox.at[fo, k], s_out, r_part.at[2 if fo else k], d_mate)

    def m0(fo, qo):
        slot = 2 * fo + qo
        lses = [lse_of([stats0[fo, d, j] for d in range(4)]) for j in range(tiles)]
        pts = xg[my_rows, :] if fo else xo[...]
        m_region(lses, slot * tiles, pts, slot * n_rows, part.at[slot, 1], part.at[slot, 0], True)

    step = n_comp // PIECES
    with jax.named_scope("w_st0_0"):
        st0_copy(0).wait_recv()
    with jax.named_scope("m0_0"):
        m0(0, 0)
    for k in range(2):
        part_copy(0, k).start()
    with jax.named_scope("m0_1"):
        m0(0, 1)
    with jax.named_scope("w_x0"):
        xs[0].wait_recv()
    over_y.start()
    relays[0].start()
    with jax.named_scope("w_part0"):
        part_copy(0, 0).wait_recv()
    sums = []
    for p in range(PIECES):
        at = pl.ds(p * step, step)
        xsend[at, :] = (part[1, 0, at, :] + inbox[0, 0, at, :]).astype(BF16)
        c = remote(xsend.at[at, :], xin.at[at, :], s_out, r_xs, d_across)
        c.start()
        sums.append(c)
    part_copy(0, 1).wait_recv()
    flat = jnp.sum(jnp.transpose(part[1, 1] + inbox[0, 1]), axis=0, keepdims=True)
    for h in range(n_comp // LANES):
        nsend[h:h + 1, :] = flat[:, h * LANES:(h + 1) * LANES]
    counts = remote(nsend, nin, s_out, r_n, d_across)
    counts.start()
    with jax.named_scope("w_st0_1"):
        st0_copy(1).wait_recv()
    with jax.named_scope("m0_2"):
        m0(1, 0)
    for k in range(2):
        part_copy(1, k).start()
    with jax.named_scope("m0_3"):
        m0(1, 1)
    for p in range(1, len(xs)):
        with jax.named_scope(f"w_x{p}"):
            xs[p].wait_recv()
        relays[p].start()
    with jax.named_scope("w_part1"):
        drain(inbox.at[1], r_part.at[2])
    with jax.named_scope("w_y"):
        over_y.wait_recv()
    relays[-1].start()
    with jax.named_scope("w_xin"):
        counts.wait_recv()
        drain(xsend, r_xs)
    n_across = column(jnp.concatenate([nin[h:h + 1, :] for h in range(n_comp // LANES)], axis=1))
    ssum[...] = part[3, 0] + inbox[1, 0] + xin[...].astype(F32)
    n_first = jnp.sum(part[3, 1] + inbox[1, 1], axis=1, keepdims=True) + n_across

    def cross(t):
        return lax.dot_general(mub[...], xg[pl.ds(pl.multiple_of(t * TILE, TILE), TILE), :], NT,
                               preferred_element_type=F32)

    def st_send(sweep, group):
        t, count, sem = group[:3]
        at = stats.at[sweep - 1, me, pl.ds(t, count)]
        for dev in (d_y, d_y_mate, d_mate):
            remote(at, at, s_out, r_st.at[sweep - 1, sem], dev).start()

    def e_group(sweep, *groups):
        todo = [t + i for t, count, _ in groups for i in range(count)]
        ahead = cross(todo[0])
        for i, t in enumerate(todo):
            a = ahead
            if i + 1 < len(todo):
                ahead = cross(todo[i + 1])
            e_tile(sweep, t, a, cc, stats.at[sweep - 1, me, t])
        for group in groups:
            st_send(sweep, group)

    def m_group(sweep, t, count, sems, at, first, after=None):
        with jax.named_scope("stwait"):
            for sem in sems:
                drain(stats.at[sweep - 1, pl.ds(0, 3), pl.ds(0, count // len(sems))], r_st.at[sweep - 1, sem])
        with jax.named_scope("mgroup"):
            lses = []
            for j in range(count):
                lses.append(lse_of([stats[sweep - 1, d, t + j] for d in range(4)]))
                lse2[t + j] = lses[-1]
            pts = xg[pl.ds(pl.multiple_of(t * TILE, TILE), count * TILE), :]
            if after is None:
                m_region(lses, t, pts, at, nacc, ssum, first)
            else:
                for lo in range(0, n_comp, n_comp // 2):
                    m_region(lses, t, pts, at, nacc, ssum, first, lo, lo + n_comp // 2)
                    after(lo, lo + n_comp // 2)

    def finish(n):
        mean = ssum[...] / (n + EPS_COUNT)
        logw = jnp.log((n + PRIOR_ALPHA) / (total_pts + total_comp * PRIOR_ALPHA))
        return mean, logw

    def piece(fit, one, p):
        return mu_out.at[fit, pl.ds(pl.multiple_of(one * n_comp + p * step, step), step), :]

    def send_final(lo, hi):
        n = jnp.sum(nacc[lo:hi, :], axis=1, keepdims=True)
        mu_out[x, pl.ds(pl.multiple_of(core * n_comp + lo, step), hi - lo), :] = ssum[lo:hi, :] / (n + EPS_COUNT)
        for p in range(lo // step, hi // step):
            remote(piece(x, core, p), piece(x, core, p), s_out, r_fin.at[p], d_across_one).start()

    with jax.named_scope("finish"):
        mean, logw = finish(n_first)
        means_to(1, mean, logw, mub, cc)
    for sweep in range(1, sweeps):
        if sweep == 1:
            near, far = 2 * x * tiles, 2 * (1 - x) * tiles
            with jax.named_scope("w_own"):
                own.wait_recv()
            with jax.named_scope("e_near"):
                e_group(1, (near, 2 * tiles, 0))
            with jax.named_scope("w_rel"):
                drain(xo, r_rel)
            with jax.named_scope("e_far"):
                e_group(1, (far, 2 * tiles, 1))
            m_group(1, near, 2 * tiles, (0,), 0, True)
            m_group(1, far, 2 * tiles, (1,), 2 * n_rows, False)
        else:
            n_tiles = blocks * tiles
            with jax.named_scope("esweep"):
                e_group(sweep, (0, FIRST, 0))
                e_group(sweep, (FIRST, n_tiles - FIRST, 1))
            m_group(sweep, 0, FIRST, (0,), 0, True)
            m_group(sweep, FIRST, n_tiles - FIRST, (1,), FIRST * TILE, False,
                    send_final if sweep == sweeps - 1 else None)
        if sweep < sweeps - 1:
            with jax.named_scope("finish"):
                mean, logw = finish(jnp.sum(nacc[...], axis=1, keepdims=True))
                means_to(sweep + 1, mean, logw, mub, cc)

    whole = mu_out.at[x, my_comps, :]
    to_mate = remote(whole, whole, s_out, r_mate, d_mate)
    to_mate.start()
    last = remote(lse2.at[pl.ds(across * tiles, tiles)], lse_in, s_out, r_lse, d_across)
    last.start()
    n_last = jnp.sum(jnp.transpose(nacc[...]), axis=0, keepdims=True)
    flat = jnp.log((n_last + PRIOR_ALPHA) / (total_pts + total_comp * PRIOR_ALPHA))
    for h in range(n_comp // LANES):
        aux[row, h:h + 1, :] = flat[:, h * LANES:(h + 1) * LANES]
    auxs = []
    for k, dev in enumerate((d_mate, d_across, d_across_mate)):
        c = remote(aux.at[row], aux.at[row], s_out, r_aux, dev)
        c.start()
        auxs.append(c)

    ones = jnp.ones((8, LANES), BF16)

    def sq_rows(pts):
        xf = pts.astype(F32)
        xx = xf * xf
        hi = xx.astype(BF16)
        lo = (xx - hi.astype(F32)).astype(BF16)
        sq = lax.dot_general(ones, hi, NT, preferred_element_type=F32)
        return sq + lax.dot_general(ones, lo, NT, preferred_element_type=F32)

    def write_lse(sq_own, sq_other):
        for s in range(2):
            sq = jnp.where(x == s, sq_own, sq_other)
            for j in range(tiles):
                val = jnp.where(x == s, lse2[row * tiles + j], lse_in[j])
                for h in range(halves):
                    at = slice(j * TILE + h * LANES, j * TILE + (h + 1) * LANES)
                    lse_out[s:s + 1, at] = val[h:h + 1, :] * LN2 - temp_ref[sweeps - 1] * sq[0:1, at]

    with jax.named_scope("lse"):
        sq_own = sq_rows(xg[my_rows, :])
        sq_other = sq_rows(xo[...])
    @pl.when(core == 1)
    def _():
        for p in range(PIECES):
            with jax.named_scope(f"w_fin{p}"):
                drain(ssum.at[pl.ds(0, 2 * step)], r_fin.at[p])
            for one in range(2):
                got = piece(1 - x, one, p)
                remote(got, got, s_out, r_frl, d_mate).start()

    with jax.named_scope("w_last"):
        last.wait_recv()
    write_lse(sq_own, sq_other)
    drain(aux.at[pl.ds(0, 3)], r_aux)
    for b in range(blocks):
        for h in range(n_comp // LANES):
            at = (b % 2) * n_comp + h * LANES
            lp_out[b // 2:b // 2 + 1, at:at + LANES] = aux[b, h:h + 1, :]
    with jax.named_scope("w_frel"):
        to_mate.wait_recv()

        @pl.when(core == 0)
        def _():
            drain(mu_out.at[0], r_frl)

    with jax.named_scope("w_sends"):
        for c in (own, to_mate, last, counts, over_y):
            c.wait_send()
        drain(stats0.at[:, pl.ds(0, 2)], s_out)
        drain(part.at[pl.ds(0, 2)], s_out)
        drain(xsend, s_out)
        drain(xo.at[pl.ds(0, (both + SHARED) * unit), :], s_out)
        drain(xo, s_out)
        drain(ssum, s_out)

        @pl.when(core == 1)
        def _():
            drain(mu_out.at[0], s_out)

        drain(aux.at[pl.ds(0, 3)], s_out)
        drain(stats.at[:, pl.ds(0, 3)], s_out)


def store_kernel(a, b, c, a_out, b_out, c_out, sem):
    copies = [
        pltpu.make_async_copy(src, dst, sem.at[i])
        for i, (src, dst) in enumerate(((a, a_out), (b, b_out), (c, c_out)))
    ]
    for c in copies:
        c.start()
    for c in copies:
        c.wait()


def solution(mesh):
    rows_size = mesh.shape["row"]
    comp_size = mesh.shape["comp"]

    def local_fit(x_local, mu_init, logpi_init, inv_temp):
        n_rows = x_local.shape[0]
        half = x_local.shape[1] // 2
        n_half = mu_init.shape[1]
        n_comp = n_half // 2
        sweeps = inv_temp.shape[0]
        total_pts = n_rows * rows_size
        n_tiles = total_pts // TILE
        tiles = n_rows // TILE
        halves = TILE // LANES
        vmem = pl.BlockSpec(memory_space=pltpu.VMEM)
        hbm = pl.BlockSpec(memory_space=pl.ANY)
        dma = pltpu.SemaphoreType.DMA
        outs = pl.pallas_call(
            functools.partial(em_kernel, sweeps, total_pts, n_half * comp_size),
            out_shape=(
                pltpu.VMEM(mu_init.shape, F32),
                pltpu.VMEM(logpi_init.shape, F32),
                pltpu.VMEM((2, n_rows), F32),
            ),
            in_specs=[hbm] * 4,
            out_specs=(vmem, vmem, vmem),
            scratch_shapes=[
                pltpu.SMEM((sweeps,), F32),
                pltpu.VMEM((n_rows, half), BF16),
                pltpu.VMEM((total_pts, half), BF16),
                pltpu.VMEM(mu_init.shape, F32),
                pltpu.VMEM(logpi_init.shape, F32),
                pltpu.VMEM((4, n_comp, half), BF16),
                pltpu.VMEM((4, n_comp, LANES), F32),
                pltpu.VMEM((2, 4, tiles, halves, LANES), F32),
                pltpu.VMEM((4, 2, n_comp, LANES), F32),
                pltpu.VMEM((2, 2, n_comp, LANES), F32),
                pltpu.VMEM((n_comp, half), BF16),
                pltpu.VMEM((n_comp, half), BF16),
                pltpu.VMEM((n_comp // LANES, LANES), F32),
                pltpu.VMEM((n_comp // LANES, LANES), F32),
                pltpu.VMEM((n_comp, half), BF16),
                pltpu.VMEM((n_comp, LANES), F32),
                pltpu.VMEM((n_tiles, n_comp, TILE), F32),
                pltpu.VMEM((n_tiles, halves, LANES), F32),
                pltpu.VMEM((sweeps - 1, 4, n_tiles, halves, LANES), F32),
                pltpu.VMEM((n_comp, total_pts), BF16),
                pltpu.VMEM((n_comp, half), F32),
                pltpu.VMEM((n_comp, LANES), F32),
                pltpu.VMEM((n_tiles, halves, LANES), F32),
                pltpu.VMEM((tiles, halves, LANES), F32),
                pltpu.VMEM((rows_size, n_comp // LANES, LANES), F32),
                dma((6,)), dma, dma, dma((3,)), dma, dma, dma((2,)), dma((3,)), dma, dma,
                dma((sweeps - 1, 2)), dma, dma((PIECES,)), dma, dma, dma,
            ],
            compiler_params=pltpu.CompilerParams(collective_id=0, has_side_effects=True),
        )(inv_temp, x_local, mu_init, logpi_init)
        outs = [pltpu.with_memory_space_constraint(o, pltpu.VMEM) for o in outs]
        return pl.pallas_call(
            store_kernel,
            out_shape=tuple(jax.ShapeDtypeStruct(o.shape, F32) for o in outs),
            in_specs=[vmem] * 3,
            out_specs=(hbm, hbm, hbm),
            scratch_shapes=[dma((3,))],
        )(*outs)

    return jax.shard_map(
        local_fit,
        mesh=mesh,
        in_specs=(P(("grp", "row"), None), P(None, ("grp", "comp"), None), P(None, ("grp", "comp")), P()),
        out_specs=(P(None, ("grp", "comp"), None), P(None, ("grp", "comp")), P(None, ("grp", "row"))),
        check_vma=False,
    )
```

```python
import functools

import jax
import jax.numpy as jnp
from jax import lax
from jax.experimental import pallas as pl
from jax.experimental.pallas import tpu as pltpu
from jax.sharding import PartitionSpec as P

EPS_COUNT = 1e-6
PRIOR_ALPHA = 1e-3
LOG2E = 1.4426950408889634
LN2 = 0.6931471805599453
LANES = 128
TILE = 256
FIRST = 9
PIECES = 8
SHARED = 3

MESH = pl.DeviceIdType.MESH
F32 = jnp.float32
BF16 = jnp.bfloat16
NT = (((1,), (1,)), ((), ()))


def em_kernel(
    sweeps, total_pts, total_comp,
    temp_in, x_in, mu_in, lp_in,
    mu_out, lp_out, lse_out,
    temp_ref, xo, xg, mu0, lp0, mub0, cc0, stats0, part, inbox, xsend, xin, nsend, nin,
    mub, cc, ee, mm, stats, rr, ssum, nacc, lse2, lse_in, aux,
    s_in, s_out, r_own, r_x, r_y, r_rel, r_st0, r_part, r_xs, r_n, r_st, r_lse, r_fin, r_mate, r_frl, r_aux,
):
    row = lax.axis_index("row")
    y = lax.axis_index("comp")
    x = row // 2
    core = row % 2
    me = 2 * y + core
    mate = 2 * x + 1 - core
    across = 2 * (1 - x) + core
    across_mate = 2 * (1 - x) + 1 - core
    across_one = 2 * (1 - x) + 1

    n_rows = xo.shape[0]
    n_comp = mub.shape[0]
    blocks = xg.shape[0] // n_rows
    tiles = n_rows // TILE
    halves = TILE // LANES
    fit_col = pl.ds(pl.multiple_of(x * LANES, LANES), LANES)
    other_col = pl.ds(pl.multiple_of((1 - x) * LANES, LANES), LANES)
    my_comps = pl.ds(pl.multiple_of(core * n_comp, n_comp), n_comp)
    mates_comps = pl.ds(pl.multiple_of((1 - core) * n_comp, n_comp), n_comp)
    my_rows = pl.ds(pl.multiple_of(row * n_rows, n_rows), n_rows)

    d_mate = {"row": mate}
    d_across = {"row": across}
    d_across_mate = {"row": across_mate}
    d_across_one = {"row": across_one}
    d_y = {"comp": 1 - y}
    d_y_mate = {"comp": 1 - y, "row": mate}

    def drain(ref, sem):
        pltpu.make_async_copy(ref, ref, sem).wait()

    def remote(src, dst, ssem, rsem, dev):
        return pltpu.make_async_remote_copy(src, dst, ssem, rsem, device_id=dev, device_id_type=MESH)

    loads = [
        pltpu.make_async_copy(src, dst, s_in.at[i])
        for i, (src, dst) in enumerate((
            (x_in.at[:, other_col], xo),
            (mu_in.at[1 - x], mu0.at[1 - x]),
            (lp_in, lp0),
            (temp_in, temp_ref),
            (x_in.at[:, fit_col], xg.at[my_rows, :]),
            (mu_in.at[x], mu0.at[x]),
        ))
    ]
    barrier = pltpu.get_barrier_semaphore()
    for dev in (d_mate, d_across, d_across_mate, d_y, d_y_mate):
        pl.semaphore_signal(barrier, inc=1, device_id=dev, device_id_type=MESH)
    for c in loads[:4]:
        c.start()
    with jax.named_scope("barrier"):
        pl.semaphore_wait(barrier, 5)
    for c in loads[4:]:
        c.start()
    with jax.named_scope("loads"):
        loads[0].wait()

    def rows_of(block, j):
        return pl.ds(pl.multiple_of(block * n_rows + j * TILE, TILE), TILE)

    unit = n_rows // 16
    both = 16 - 2 * SHARED
    once = both + SHARED * y
    chunks = ((once, SHARED), (0, both // 2), (both // 2, both - both // 2))

    def some_rows(block, first, count):
        return pl.ds(pl.multiple_of(block * n_rows + first * unit, unit), count * unit)

    xs, relays = [], []
    for p, (first, count) in enumerate(chunks):
        xs.append(remote(xo.at[some_rows(0, first, count), :], xg.at[some_rows(row, first, count), :],
                         s_out, r_x.at[p], d_across))
        got = xg.at[some_rows(across, first, count), :]
        relays.append(remote(got, got, s_out, r_rel, d_mate))
    got = xg.at[some_rows(across, once, SHARED), :]
    over_y = remote(got, got, s_out, r_y, d_y)
    got = xg.at[some_rows(across, both + SHARED * (1 - y), SHARED), :]
    relays.append(remote(got, got, s_out, r_rel, d_mate))
    own = remote(xg.at[my_rows, :], xg.at[my_rows, :], s_out, r_own, d_mate)
    for c in xs:
        c.start()
    for c in loads[1:4]:
        c.wait()

    def means_to(sweep, mean, logw, mub_at, cc_at):
        mub_at[...] = mean.astype(BF16)
        sq = jnp.sum(mean * mean, axis=1, keepdims=True)
        cc_at[...] = jnp.broadcast_to(LOG2E * (logw - temp_ref[sweep] * sq), cc_at.shape)

    def column(flat):
        return jnp.transpose(jnp.broadcast_to(flat, (LANES, n_comp)))

    def e_tile(sweep, t, a, cc_at, stat):
        scale = (2.0 * LOG2E) * temp_ref[sweep]
        for h in range(halves):
            z = a[:, h * LANES:(h + 1) * LANES] * scale + cc_at[...]
            m = jnp.max(z, axis=0, keepdims=True)
            e = jnp.exp2(z - m)
            r = jnp.sum(e, axis=0, keepdims=True)
            ee[t, :, h * LANES:(h + 1) * LANES] = e
            mm[t, h:h + 1, :] = m
            stat[h:h + 1, :] = m + jnp.log2(r)

    def lse_of(parts):
        top = jnp.maximum(jnp.maximum(parts[0], parts[1]), jnp.maximum(parts[2], parts[3]))
        tot = (jnp.exp2(parts[0] - top) + jnp.exp2(parts[1] - top)) + (
            jnp.exp2(parts[2] - top) + jnp.exp2(parts[3] - top))
        return top + jnp.log2(tot)

    def m_region(lses, base, pts, at, n_at, s_at, first, lo=0, hi=n_comp):
        ws = []
        for j, lse in enumerate(lses):
            w = jnp.exp2(mm[base + j] - lse)
            ws += [w[h:h + 1, :] for h in range(halves)]
        for k in range(lo, hi, 16):
            acc = None if first else n_at[k:k + 16, :]
            for v, w in enumerate(ws):
                r = ee[base + v // halves, k:k + 16, (v % halves) * LANES:(v % halves + 1) * LANES] * w
                acc = r if acc is None else acc + r
                rr[k:k + 16, at + v * LANES:at + (v + 1) * LANES] = r.astype(BF16)
            n_at[k:k + 16, :] = acc
        s = jnp.dot(rr[lo:hi, at:at + len(lses) * TILE], pts, preferred_element_type=F32)
        if first:
            s_at[lo:hi, :] = s
        else:
            s_at[lo:hi, :] += s

    def cross0(slot, j):
        pts = xg[rows_of(row, j), :] if slot // 2 else xo[pl.ds(j * TILE, TILE), :]
        return lax.dot_general(mub0[slot], pts, NT, preferred_element_type=F32)

    def st0_copy(fo):
        at = stats0.at[fo, pl.ds(2 * y, 2)]
        return remote(at, at, s_out, r_st0.at[fo], d_y)

    for fo, fit in enumerate((1 - x, x)):
        with jax.named_scope(f"set0_{fo}"):
            for qo, comps in enumerate((mates_comps, my_comps)):
                slot = 2 * fo + qo
                means_to(0, mu0[fit, comps, :], column(lp0[pl.ds(fit, 1), comps]), mub0.at[slot], cc0.at[slot])
        with jax.named_scope(f"e0_{fo}"):
            order = [(2 * fo + qo, j) for qo in range(2) for j in range(tiles)]
            ahead = cross0(*order[0])
            for i, (slot, j) in enumerate(order):
                a = ahead
                if i + 1 < len(order):
                    ahead = cross0(*order[i + 1])
                e_tile(0, slot * tiles + j, a, cc0.at[slot], stats0.at[fo, 2 * y + slot % 2, j])
        st0_copy(fo).start()
        if fo == 0:
            for c in loads[4:]:
                c.wait()
            own.start()

    def part_copy(fo, k):
        return remote(part.at[2 * fo, k], inbox.at[fo, k], s_out, r_part.at[2 if fo else k], d_mate)

    def m0(fo, qo):
        slot = 2 * fo + qo
        lses = [lse_of([stats0[fo, d, j] for d in range(4)]) for j in range(tiles)]
        pts = xg[my_rows, :] if fo else xo[...]
        m_region(lses, slot * tiles, pts, slot * n_rows, part.at[slot, 1], part.at[slot, 0], True)

    step = n_comp // PIECES
    with jax.named_scope("w_st0_0"):
        st0_copy(0).wait_recv()
    with jax.named_scope("m0_0"):
        m0(0, 0)
    for k in range(2):
        part_copy(0, k).start()
    with jax.named_scope("m0_1"):
        m0(0, 1)
    with jax.named_scope("w_x0"):
        xs[0].wait_recv()
    over_y.start()
    relays[0].start()
    with jax.named_scope("w_part0"):
        part_copy(0, 0).wait_recv()
    sums = []
    for p in range(PIECES):
        at = pl.ds(p * step, step)
        xsend[at, :] = (part[1, 0, at, :] + inbox[0, 0, at, :]).astype(BF16)
        c = remote(xsend.at[at, :], xin.at[at, :], s_out, r_xs, d_across)
        c.start()
        sums.append(c)
    part_copy(0, 1).wait_recv()
    flat = jnp.sum(jnp.transpose(part[1, 1] + inbox[0, 1]), axis=0, keepdims=True)
    for h in range(n_comp // LANES):
        nsend[h:h + 1, :] = flat[:, h * LANES:(h + 1) * LANES]
    counts = remote(nsend, nin, s_out, r_n, d_across)
    counts.start()
    with jax.named_scope("w_st0_1"):
        st0_copy(1).wait_recv()
    with jax.named_scope("m0_2"):
        m0(1, 0)
    for k in range(2):
        part_copy(1, k).start()
    with jax.named_scope("m0_3"):
        m0(1, 1)
    for p in range(1, len(xs)):
        with jax.named_scope(f"w_x{p}"):
            xs[p].wait_recv()
        relays[p].start()
    with jax.named_scope("w_part1"):
        drain(inbox.at[1], r_part.at[2])
    with jax.named_scope("w_y"):
        over_y.wait_recv()
    relays[-1].start()
    with jax.named_scope("w_xin"):
        counts.wait_recv()
        drain(xsend, r_xs)
    n_across = column(jnp.concatenate([nin[h:h + 1, :] for h in range(n_comp // LANES)], axis=1))
    ssum[...] = part[3, 0] + inbox[1, 0] + xin[...].astype(F32)
    n_first = jnp.sum(part[3, 1] + inbox[1, 1], axis=1, keepdims=True) + n_across

    def cross(t):
        return lax.dot_general(mub[...], xg[pl.ds(pl.multiple_of(t * TILE, TILE), TILE), :], NT,
                               preferred_element_type=F32)

    def st_send(sweep, group):
        t, count, sem = group[:3]
        at = stats.at[sweep - 1, me, pl.ds(t, count)]
        for dev in (d_y, d_y_mate, d_mate):
            remote(at, at, s_out, r_st.at[sweep - 1, sem], dev).start()

    def e_group(sweep, *groups):
        todo = [t + i for t, count, _ in groups for i in range(count)]
        ahead = cross(todo[0])
        for i, t in enumerate(todo):
            a = ahead
            if i + 1 < len(todo):
                ahead = cross(todo[i + 1])
            e_tile(sweep, t, a, cc, stats.at[sweep - 1, me, t])
        for group in groups:
            st_send(sweep, group)

    def m_group(sweep, t, count, sems, at, first, after=None):
        with jax.named_scope("stwait"):
            for sem in sems:
                drain(stats.at[sweep - 1, pl.ds(0, 3), pl.ds(0, count // len(sems))], r_st.at[sweep - 1, sem])
        with jax.named_scope("mgroup"):
            lses = []
            for j in range(count):
                lses.append(lse_of([stats[sweep - 1, d, t + j] for d in range(4)]))
                lse2[t + j] = lses[-1]
            pts = xg[pl.ds(pl.multiple_of(t * TILE, TILE), count * TILE), :]
            if after is None:
                m_region(lses, t, pts, at, nacc, ssum, first)
            else:
                for lo in range(0, n_comp, n_comp // 2):
                    m_region(lses, t, pts, at, nacc, ssum, first, lo, lo + n_comp // 2)
                    after(lo, lo + n_comp // 2)

    def finish(n):
        mean = ssum[...] / (n + EPS_COUNT)
        logw = jnp.log((n + PRIOR_ALPHA) / (total_pts + total_comp * PRIOR_ALPHA))
        return mean, logw

    def piece(fit, one, p):
        return mu_out.at[fit, pl.ds(pl.multiple_of(one * n_comp + p * step, step), step), :]

    def send_final(lo, hi):
        n = jnp.sum(nacc[lo:hi, :], axis=1, keepdims=True)
        mu_out[x, pl.ds(pl.multiple_of(core * n_comp + lo, step), hi - lo), :] = ssum[lo:hi, :] / (n + EPS_COUNT)
        for p in range(lo // step, hi // step):
            remote(piece(x, core, p), piece(x, core, p), s_out, r_fin.at[p], d_across_one).start()

    with jax.named_scope("finish"):
        mean, logw = finish(n_first)
        means_to(1, mean, logw, mub, cc)
    for sweep in range(1, sweeps):
        if sweep == 1:
            near, far = 2 * x * tiles, 2 * (1 - x) * tiles
            with jax.named_scope("w_own"):
                own.wait_recv()
            with jax.named_scope("e_near"):
                e_group(1, (near, 2 * tiles, 0))
            with jax.named_scope("w_rel"):
                drain(xo, r_rel)
            with jax.named_scope("e_far"):
                e_group(1, (far, 2 * tiles, 1))
            m_group(1, near, 2 * tiles, (0,), 0, True)
            m_group(1, far, 2 * tiles, (1,), 2 * n_rows, False)
        else:
            n_tiles = blocks * tiles
            with jax.named_scope("esweep"):
                e_group(sweep, (0, FIRST, 0))
                e_group(sweep, (FIRST, n_tiles - FIRST, 1))
            m_group(sweep, 0, FIRST, (0,), 0, True)
            m_group(sweep, FIRST, n_tiles - FIRST, (1,), FIRST * TILE, False,
                    send_final if sweep == sweeps - 1 else None)
        if sweep < sweeps - 1:
            with jax.named_scope("finish"):
                mean, logw = finish(jnp.sum(nacc[...], axis=1, keepdims=True))
                means_to(sweep + 1, mean, logw, mub, cc)

    whole = mu_out.at[x, my_comps, :]
    to_mate = remote(whole, whole, s_out, r_mate, d_mate)
    to_mate.start()
    last = remote(lse2.at[pl.ds(across * tiles, tiles)], lse_in, s_out, r_lse, d_across)
    last.start()
    n_last = jnp.sum(jnp.transpose(nacc[...]), axis=0, keepdims=True)
    flat = jnp.log((n_last + PRIOR_ALPHA) / (total_pts + total_comp * PRIOR_ALPHA))
    for h in range(n_comp // LANES):
        aux[row, h:h + 1, :] = flat[:, h * LANES:(h + 1) * LANES]
    auxs = []
    for k, dev in enumerate((d_mate, d_across, d_across_mate)):
        c = remote(aux.at[row], aux.at[row], s_out, r_aux, dev)
        c.start()
        auxs.append(c)

    ones = jnp.ones((8, LANES), BF16)

    def sq_rows(pts):
        xf = pts.astype(F32)
        xx = xf * xf
        hi = xx.astype(BF16)
        lo = (xx - hi.astype(F32)).astype(BF16)
        sq = lax.dot_general(ones, hi, NT, preferred_element_type=F32)
        return sq + lax.dot_general(ones, lo, NT, preferred_element_type=F32)

    def write_lse(sq_own, sq_other):
        for s in range(2):
            sq = jnp.where(x == s, sq_own, sq_other)
            for j in range(tiles):
                val = jnp.where(x == s, lse2[row * tiles + j], lse_in[j])
                for h in range(halves):
                    at = slice(j * TILE + h * LANES, j * TILE + (h + 1) * LANES)
                    lse_out[s:s + 1, at] = val[h:h + 1, :] * LN2 - temp_ref[sweeps - 1] * sq[0:1, at]

    with jax.named_scope("lse"):
        sq_own = sq_rows(xg[my_rows, :])
        sq_other = sq_rows(xo[...])
    @pl.when(core == 1)
    def _():
        for p in range(PIECES):
            with jax.named_scope(f"w_fin{p}"):
                drain(ssum.at[pl.ds(0, 2 * step)], r_fin.at[p])
            for one in range(2):
                got = piece(1 - x, one, p)
                remote(got, got, s_out, r_frl, d_mate).start()

    with jax.named_scope("w_last"):
        last.wait_recv()
    write_lse(sq_own, sq_other)
    drain(aux.at[pl.ds(0, 3)], r_aux)
    for b in range(blocks):
        for h in range(n_comp // LANES):
            at = (b % 2) * n_comp + h * LANES
            lp_out[b // 2:b // 2 + 1, at:at + LANES] = aux[b, h:h + 1, :]
    with jax.named_scope("w_frel"):
        to_mate.wait_recv()

        @pl.when(core == 0)
        def _():
            drain(mu_out.at[0], r_frl)

    with jax.named_scope("w_sends"):
        for c in (own, to_mate, last, counts, over_y):
            c.wait_send()
        drain(stats0.at[:, pl.ds(0, 2)], s_out)
        drain(part.at[pl.ds(0, 2)], s_out)
        drain(xsend, s_out)
        drain(xo.at[pl.ds(0, (both + SHARED) * unit), :], s_out)
        drain(xo, s_out)
        drain(ssum, s_out)

        @pl.when(core == 1)
        def _():
            drain(mu_out.at[0], s_out)

        drain(aux.at[pl.ds(0, 3)], s_out)
        drain(stats.at[:, pl.ds(0, 3)], s_out)


def store_kernel(a, b, c, a_out, b_out, c_out, sem):
    copies = [
        pltpu.make_async_copy(src, dst, sem.at[i])
        for i, (src, dst) in enumerate(((a, a_out), (b, b_out), (c, c_out)))
    ]
    for c in copies:
        c.start()
    for c in copies:
        c.wait()


def solution(mesh):
    rows_size = mesh.shape["row"]
    comp_size = mesh.shape["comp"]

    def local_fit(x_local, mu_init, logpi_init, inv_temp):
        n_rows = x_local.shape[0]
        half = x_local.shape[1] // 2
        n_half = mu_init.shape[1]
        n_comp = n_half // 2
        sweeps = inv_temp.shape[0]
        total_pts = n_rows * rows_size
        n_tiles = total_pts // TILE
        tiles = n_rows // TILE
        halves = TILE // LANES
        vmem = pl.BlockSpec(memory_space=pltpu.VMEM)
        hbm = pl.BlockSpec(memory_space=pl.ANY)
        dma = pltpu.SemaphoreType.DMA
        outs = pl.pallas_call(
            functools.partial(em_kernel, sweeps, total_pts, n_half * comp_size),
            out_shape=(
                pltpu.VMEM(mu_init.shape, F32),
                pltpu.VMEM(logpi_init.shape, F32),
                pltpu.VMEM((2, n_rows), F32),
            ),
            in_specs=[hbm] * 4,
            out_specs=(vmem, vmem, vmem),
            scratch_shapes=[
                pltpu.SMEM((sweeps,), F32),
                pltpu.VMEM((n_rows, half), BF16),
                pltpu.VMEM((total_pts, half), BF16),
                pltpu.VMEM(mu_init.shape, F32),
                pltpu.VMEM(logpi_init.shape, F32),
                pltpu.VMEM((4, n_comp, half), BF16),
                pltpu.VMEM((4, n_comp, LANES), F32),
                pltpu.VMEM((2, 4, tiles, halves, LANES), F32),
                pltpu.VMEM((4, 2, n_comp, LANES), F32),
                pltpu.VMEM((2, 2, n_comp, LANES), F32),
                pltpu.VMEM((n_comp, half), BF16),
                pltpu.VMEM((n_comp, half), BF16),
                pltpu.VMEM((n_comp // LANES, LANES), F32),
                pltpu.VMEM((n_comp // LANES, LANES), F32),
                pltpu.VMEM((n_comp, half), BF16),
                pltpu.VMEM((n_comp, LANES), F32),
                pltpu.VMEM((n_tiles, n_comp, TILE), F32),
                pltpu.VMEM((n_tiles, halves, LANES), F32),
                pltpu.VMEM((sweeps - 1, 4, n_tiles, halves, LANES), F32),
                pltpu.VMEM((n_comp, total_pts), BF16),
                pltpu.VMEM((n_comp, half), F32),
                pltpu.VMEM((n_comp, LANES), F32),
                pltpu.VMEM((n_tiles, halves, LANES), F32),
                pltpu.VMEM((tiles, halves, LANES), F32),
                pltpu.VMEM((rows_size, n_comp // LANES, LANES), F32),
                dma((6,)), dma, dma, dma((3,)), dma, dma, dma((2,)), dma((3,)), dma, dma,
                dma((sweeps - 1, 2)), dma, dma((PIECES,)), dma, dma, dma,
            ],
            compiler_params=pltpu.CompilerParams(collective_id=0, has_side_effects=True),
        )(inv_temp, x_local, mu_init, logpi_init)
        outs = [pltpu.with_memory_space_constraint(o, pltpu.VMEM) for o in outs]
        return pl.pallas_call(
            store_kernel,
            out_shape=tuple(jax.ShapeDtypeStruct(o.shape, F32) for o in outs),
            in_specs=[vmem] * 3,
            out_specs=(hbm, hbm, hbm),
            scratch_shapes=[dma((3,))],
        )(*outs)

    return jax.shard_map(
        local_fit,
        mesh=mesh,
        in_specs=(P(("grp", "row"), None), P(None, ("grp", "comp"), None), P(None, ("grp", "comp")), P()),
        out_specs=(P(None, ("grp", "comp"), None), P(None, ("grp", "comp")), P(None, ("grp", "row"))),
        check_vma=False,
    )
```

```python
import functools

import jax
import jax.numpy as jnp
from jax import lax
from jax.experimental import pallas as pl
from jax.experimental.pallas import tpu as pltpu
from jax.sharding import PartitionSpec as P

EPS_COUNT = 1e-6
PRIOR_ALPHA = 1e-3
LOG2E = 1.4426950408889634
LN2 = 0.6931471805599453
LANES = 128
TILE = 256
FIRST = 9
PIECES = 8
SHARED = 3

MESH = pl.DeviceIdType.MESH
F32 = jnp.float32
BF16 = jnp.bfloat16
NT = (((1,), (1,)), ((), ()))


def em_kernel(
    sweeps, total_pts, total_comp,
    temp_in, x_in, mu_in, lp_in,
    mu_out, lp_out, lse_out,
    temp_ref, xo, xg, mu0, lp0, mub0, cc0, stats0, part, inbox, xsend, xin, nsend, nin,
    mub, cc, ee, mm, stats, rr, ssum, nacc, lse2, lse_in, aux,
    s_in, s_out, r_own, r_x, r_y, r_rel, r_st0, r_part, r_xs, r_n, r_st, r_lse, r_fin, r_mate, r_frl, r_aux,
):
    row = lax.axis_index("row")
    y = lax.axis_index("comp")
    x = row // 2
    core = row % 2
    me = 2 * y + core
    mate = 2 * x + 1 - core
    across = 2 * (1 - x) + core
    across_mate = 2 * (1 - x) + 1 - core
    across_one = 2 * (1 - x) + 1

    n_rows = xo.shape[0]
    n_comp = mub.shape[0]
    blocks = xg.shape[0] // n_rows
    tiles = n_rows // TILE
    halves = TILE // LANES
    fit_col = pl.ds(pl.multiple_of(x * LANES, LANES), LANES)
    other_col = pl.ds(pl.multiple_of((1 - x) * LANES, LANES), LANES)
    my_comps = pl.ds(pl.multiple_of(core * n_comp, n_comp), n_comp)
    mates_comps = pl.ds(pl.multiple_of((1 - core) * n_comp, n_comp), n_comp)
    my_rows = pl.ds(pl.multiple_of(row * n_rows, n_rows), n_rows)

    d_mate = {"row": mate}
    d_across = {"row": across}
    d_across_mate = {"row": across_mate}
    d_across_one = {"row": across_one}
    d_y = {"comp": 1 - y}
    d_y_mate = {"comp": 1 - y, "row": mate}

    def drain(ref, sem):
        pltpu.make_async_copy(ref, ref, sem).wait()

    def remote(src, dst, ssem, rsem, dev):
        return pltpu.make_async_remote_copy(src, dst, ssem, rsem, device_id=dev, device_id_type=MESH)

    loads = [
        pltpu.make_async_copy(src, dst, s_in.at[i])
        for i, (src, dst) in enumerate((
            (x_in.at[:, other_col], xo),
            (mu_in.at[1 - x], mu0.at[1 - x]),
            (lp_in, lp0),
            (temp_in, temp_ref),
            (x_in.at[:, fit_col], xg.at[my_rows, :]),
            (mu_in.at[x], mu0.at[x]),
        ))
    ]
    barrier = pltpu.get_barrier_semaphore()
    for dev in (d_mate, d_across, d_across_mate, d_y, d_y_mate):
        pl.semaphore_signal(barrier, inc=1, device_id=dev, device_id_type=MESH)
    for c in loads[:4]:
        c.start()
    with jax.named_scope("barrier"):
        pl.semaphore_wait(barrier, 5)
    for c in loads[4:]:
        c.start()
    with jax.named_scope("loads"):
        loads[0].wait()

    def rows_of(block, j):
        return pl.ds(pl.multiple_of(block * n_rows + j * TILE, TILE), TILE)

    unit = n_rows // 16
    both = 16 - 2 * SHARED
    once = both + SHARED * y
    chunks = ((once, SHARED), (0, both // 2), (both // 2, both - both // 2))

    def some_rows(block, first, count):
        return pl.ds(pl.multiple_of(block * n_rows + first * unit, unit), count * unit)

    xs, relays = [], []
    for p, (first, count) in enumerate(chunks):
        xs.append(remote(xo.at[some_rows(0, first, count), :], xg.at[some_rows(row, first, count), :],
                         s_out, r_x.at[p], d_across))
        got = xg.at[some_rows(across, first, count), :]
        relays.append(remote(got, got, s_out, r_rel, d_mate))
    got = xg.at[some_rows(across, once, SHARED), :]
    over_y = remote(got, got, s_out, r_y, d_y)
    got = xg.at[some_rows(across, both + SHARED * (1 - y), SHARED), :]
    relays.append(remote(got, got, s_out, r_rel, d_mate))
    own = remote(xg.at[my_rows, :], xg.at[my_rows, :], s_out, r_own, d_mate)
    for c in xs:
        c.start()
    for c in loads[1:4]:
        c.wait()

    def means_to(sweep, mean, logw, mub_at, cc_at):
        mub_at[...] = mean.astype(BF16)
        sq = jnp.sum(mean * mean, axis=1, keepdims=True)
        cc_at[...] = jnp.broadcast_to(LOG2E * (logw - temp_ref[sweep] * sq), cc_at.shape)

    def column(flat):
        return jnp.transpose(jnp.broadcast_to(flat, (LANES, n_comp)))

    def e_tile(sweep, t, a, cc_at, stat):
        scale = (2.0 * LOG2E) * temp_ref[sweep]
        for h in range(halves):
            z = a[:, h * LANES:(h + 1) * LANES] * scale + cc_at[...]
            m = jnp.max(z, axis=0, keepdims=True)
            e = jnp.exp2(z - m)
            r = jnp.sum(e, axis=0, keepdims=True)
            ee[t, :, h * LANES:(h + 1) * LANES] = e
            mm[t, h:h + 1, :] = m
            stat[h:h + 1, :] = m + jnp.log2(r)

    def lse_of(parts):
        top = jnp.maximum(jnp.maximum(parts[0], parts[1]), jnp.maximum(parts[2], parts[3]))
        tot = (jnp.exp2(parts[0] - top) + jnp.exp2(parts[1] - top)) + (
            jnp.exp2(parts[2] - top) + jnp.exp2(parts[3] - top))
        return top + jnp.log2(tot)

    def m_region(lses, base, pts, at, n_at, s_at, first, lo=0, hi=n_comp):
        ws = []
        for j, lse in enumerate(lses):
            w = jnp.exp2(mm[base + j] - lse)
            ws += [w[h:h + 1, :] for h in range(halves)]
        for k in range(lo, hi, 16):
            acc = None if first else n_at[k:k + 16, :]
            for v, w in enumerate(ws):
                r = ee[base + v // halves, k:k + 16, (v % halves) * LANES:(v % halves + 1) * LANES] * w
                acc = r if acc is None else acc + r
                rr[k:k + 16, at + v * LANES:at + (v + 1) * LANES] = r.astype(BF16)
            n_at[k:k + 16, :] = acc
        s = jnp.dot(rr[lo:hi, at:at + len(lses) * TILE], pts, preferred_element_type=F32)
        if first:
            s_at[lo:hi, :] = s
        else:
            s_at[lo:hi, :] += s

    def cross0(slot, j):
        pts = xg[rows_of(row, j), :] if slot // 2 else xo[pl.ds(j * TILE, TILE), :]
        return lax.dot_general(mub0[slot], pts, NT, preferred_element_type=F32)

    def st0_copy(fo):
        at = stats0.at[fo, pl.ds(2 * y, 2)]
        return remote(at, at, s_out, r_st0.at[fo], d_y)

    for fo, fit in enumerate((1 - x, x)):
        with jax.named_scope(f"set0_{fo}"):
            for qo, comps in enumerate((mates_comps, my_comps)):
                slot = 2 * fo + qo
                means_to(0, mu0[fit, comps, :], column(lp0[pl.ds(fit, 1), comps]), mub0.at[slot], cc0.at[slot])
        with jax.named_scope(f"e0_{fo}"):
            order = [(2 * fo + qo, j) for qo in range(2) for j in range(tiles)]
            ahead = cross0(*order[0])
            for i, (slot, j) in enumerate(order):
                a = ahead
                if i + 1 < len(order):
                    ahead = cross0(*order[i + 1])
                e_tile(0, slot * tiles + j, a, cc0.at[slot], stats0.at[fo, 2 * y + slot % 2, j])
        st0_copy(fo).start()
        if fo == 0:
            for c in loads[4:]:
                c.wait()
            own.start()

    def part_copy(fo, k):
        return remote(part.at[2 * fo, k], inbox.at[fo, k], s_out, r_part.at[2 if fo else k], d_mate)

    def m0(fo, qo):
        slot = 2 * fo + qo
        lses = [lse_of([stats0[fo, d, j] for d in range(4)]) for j in range(tiles)]
        pts = xg[my_rows, :] if fo else xo[...]
        m_region(lses, slot * tiles, pts, slot * n_rows, part.at[slot, 1], part.at[slot, 0], True)

    step = n_comp // PIECES
    with jax.named_scope("w_st0_0"):
        st0_copy(0).wait_recv()
    with jax.named_scope("m0_0"):
        m0(0, 0)
    for k in range(2):
        part_copy(0, k).start()
    with jax.named_scope("m0_1"):
        m0(0, 1)
    with jax.named_scope("w_x0"):
        xs[0].wait_recv()
    over_y.start()
    relays[0].start()
    with jax.named_scope("w_part0"):
        part_copy(0, 0).wait_recv()
    sums = []
    for p in range(2):
        at = pl.ds(p * (n_comp // 2), n_comp // 2)
        xsend[at, :] = (part[1, 0, at, :] + inbox[0, 0, at, :]).astype(BF16)
        c = remote(xsend.at[at, :], xin.at[at, :], s_out, r_xs, d_across)
        c.start()
        sums.append(c)
    part_copy(0, 1).wait_recv()
    flat = jnp.sum(jnp.transpose(part[1, 1] + inbox[0, 1]), axis=0, keepdims=True)
    for h in range(n_comp // LANES):
        nsend[h:h + 1, :] = flat[:, h * LANES:(h + 1) * LANES]
    counts = remote(nsend, nin, s_out, r_n, d_across)
    counts.start()
    with jax.named_scope("w_st0_1"):
        st0_copy(1).wait_recv()
    with jax.named_scope("m0_2"):
        m0(1, 0)
    for k in range(2):
        part_copy(1, k).start()
    with jax.named_scope("m0_3"):
        m0(1, 1)
    for p in range(1, len(xs)):
        with jax.named_scope(f"w_x{p}"):
            xs[p].wait_recv()
        relays[p].start()
    with jax.named_scope("w_part1"):
        drain(inbox.at[1], r_part.at[2])
    with jax.named_scope("w_y"):
        over_y.wait_recv()
    relays[-1].start()
    with jax.named_scope("w_xin"):
        counts.wait_recv()
        drain(xsend, r_xs)
    n_across = column(jnp.concatenate([nin[h:h + 1, :] for h in range(n_comp // LANES)], axis=1))
    ssum[...] = part[3, 0] + inbox[1, 0] + xin[...].astype(F32)
    n_first = jnp.sum(part[3, 1] + inbox[1, 1], axis=1, keepdims=True) + n_across

    def cross(t):
        return lax.dot_general(mub[...], xg[pl.ds(pl.multiple_of(t * TILE, TILE), TILE), :], NT,
                               preferred_element_type=F32)

    def st_send(sweep, group):
        t, count, sem = group[:3]
        at = stats.at[sweep - 1, me, pl.ds(t, count)]
        for dev in (d_y, d_y_mate, d_mate):
            remote(at, at, s_out, r_st.at[sweep - 1, sem], dev).start()

    def e_group(sweep, *groups):
        todo = [t + i for t, count, _ in groups for i in range(count)]
        ahead = cross(todo[0])
        for i, t in enumerate(todo):
            a = ahead
            if i + 1 < len(todo):
                ahead = cross(todo[i + 1])
            e_tile(sweep, t, a, cc, stats.at[sweep - 1, me, t])
        for group in groups:
            st_send(sweep, group)

    def m_group(sweep, t, count, sems, at, first, after=None):
        with jax.named_scope("stwait"):
            for sem in sems:
                drain(stats.at[sweep - 1, pl.ds(0, 3), pl.ds(0, count // len(sems))], r_st.at[sweep - 1, sem])
        with jax.named_scope("mgroup"):
            lses = []
            for j in range(count):
                lses.append(lse_of([stats[sweep - 1, d, t + j] for d in range(4)]))
                lse2[t + j] = lses[-1]
            pts = xg[pl.ds(pl.multiple_of(t * TILE, TILE), count * TILE), :]
            if after is None:
                m_region(lses, t, pts, at, nacc, ssum, first)
            else:
                for lo in range(0, n_comp, n_comp // 2):
                    m_region(lses, t, pts, at, nacc, ssum, first, lo, lo + n_comp // 2)
                    after(lo, lo + n_comp // 2)

    def finish(n):
        mean = ssum[...] / (n + EPS_COUNT)
        logw = jnp.log((n + PRIOR_ALPHA) / (total_pts + total_comp * PRIOR_ALPHA))
        return mean, logw

    def piece(fit, one, p):
        return mu_out.at[fit, pl.ds(pl.multiple_of(one * n_comp + p * step, step), step), :]

    def send_final(lo, hi):
        n = jnp.sum(nacc[lo:hi, :], axis=1, keepdims=True)
        mu_out[x, pl.ds(pl.multiple_of(core * n_comp + lo, step), hi - lo), :] = ssum[lo:hi, :] / (n + EPS_COUNT)
        for p in range(lo // step, hi // step):
            remote(piece(x, core, p), piece(x, core, p), s_out, r_fin.at[p], d_across_one).start()

    with jax.named_scope("finish"):
        mean, logw = finish(n_first)
        means_to(1, mean, logw, mub, cc)
    for sweep in range(1, sweeps):
        if sweep == 1:
            near, far = 2 * x * tiles, 2 * (1 - x) * tiles
            with jax.named_scope("w_own"):
                own.wait_recv()
            with jax.named_scope("e_near"):
                e_group(1, (near, 2 * tiles, 0))
            with jax.named_scope("w_rel"):
                drain(xo, r_rel)
            with jax.named_scope("e_far"):
                e_group(1, (far, 2 * tiles, 1))
            m_group(1, near, 2 * tiles, (0,), 0, True)
            m_group(1, far, 2 * tiles, (1,), 2 * n_rows, False)
        else:
            n_tiles = blocks * tiles
            with jax.named_scope("esweep"):
                e_group(sweep, (0, FIRST, 0))
                e_group(sweep, (FIRST, n_tiles - FIRST, 1))
            m_group(sweep, 0, FIRST, (0,), 0, True)
            m_group(sweep, FIRST, n_tiles - FIRST, (1,), FIRST * TILE, False,
                    send_final if sweep == sweeps - 1 else None)
        if sweep < sweeps - 1:
            with jax.named_scope("finish"):
                mean, logw = finish(jnp.sum(nacc[...], axis=1, keepdims=True))
                means_to(sweep + 1, mean, logw, mub, cc)

    whole = mu_out.at[x, my_comps, :]
    to_mate = remote(whole, whole, s_out, r_mate, d_mate)
    to_mate.start()
    last = remote(lse2.at[pl.ds(across * tiles, tiles)], lse_in, s_out, r_lse, d_across)
    last.start()
    n_last = jnp.sum(jnp.transpose(nacc[...]), axis=0, keepdims=True)
    flat = jnp.log((n_last + PRIOR_ALPHA) / (total_pts + total_comp * PRIOR_ALPHA))
    for h in range(n_comp // LANES):
        aux[row, h:h + 1, :] = flat[:, h * LANES:(h + 1) * LANES]
    auxs = []
    for k, dev in enumerate((d_mate, d_across, d_across_mate)):
        c = remote(aux.at[row], aux.at[row], s_out, r_aux, dev)
        c.start()
        auxs.append(c)

    ones = jnp.ones((8, LANES), BF16)

    def sq_rows(pts):
        xf = pts.astype(F32)
        xx = xf * xf
        hi = xx.astype(BF16)
        lo = (xx - hi.astype(F32)).astype(BF16)
        sq = lax.dot_general(ones, hi, NT, preferred_element_type=F32)
        return sq + lax.dot_general(ones, lo, NT, preferred_element_type=F32)

    def write_lse(sq_own, sq_other):
        for s in range(2):
            sq = jnp.where(x == s, sq_own, sq_other)
            for j in range(tiles):
                val = jnp.where(x == s, lse2[row * tiles + j], lse_in[j])
                for h in range(halves):
                    at = slice(j * TILE + h * LANES, j * TILE + (h + 1) * LANES)
                    lse_out[s:s + 1, at] = val[h:h + 1, :] * LN2 - temp_ref[sweeps - 1] * sq[0:1, at]

    with jax.named_scope("lse"):
        sq_own = sq_rows(xg[my_rows, :])
        sq_other = sq_rows(xo[...])
    @pl.when(core == 1)
    def _():
        for p in range(PIECES):
            with jax.named_scope(f"w_fin{p}"):
                drain(ssum.at[pl.ds(0, 2 * step)], r_fin.at[p])
            for one in range(2):
                got = piece(1 - x, one, p)
                remote(got, got, s_out, r_frl, d_mate).start()

    with jax.named_scope("w_last"):
        last.wait_recv()
    write_lse(sq_own, sq_other)
    drain(aux.at[pl.ds(0, 3)], r_aux)
    for b in range(blocks):
        for h in range(n_comp // LANES):
            at = (b % 2) * n_comp + h * LANES
            lp_out[b // 2:b // 2 + 1, at:at + LANES] = aux[b, h:h + 1, :]
    with jax.named_scope("w_frel"):
        to_mate.wait_recv()

        @pl.when(core == 0)
        def _():
            drain(mu_out.at[0], r_frl)

    with jax.named_scope("w_sends"):
        for c in (own, to_mate, last, counts, over_y):
            c.wait_send()
        drain(stats0.at[:, pl.ds(0, 2)], s_out)
        drain(part.at[pl.ds(0, 2)], s_out)
        drain(xsend, s_out)
        drain(xo.at[pl.ds(0, (both + SHARED) * unit), :], s_out)
        drain(xo, s_out)
        drain(ssum, s_out)

        @pl.when(core == 1)
        def _():
            drain(mu_out.at[0], s_out)

        drain(aux.at[pl.ds(0, 3)], s_out)
        drain(stats.at[:, pl.ds(0, 3)], s_out)


def store_kernel(a, b, c, a_out, b_out, c_out, sem):
    copies = [
        pltpu.make_async_copy(src, dst, sem.at[i])
        for i, (src, dst) in enumerate(((a, a_out), (b, b_out), (c, c_out)))
    ]
    for c in copies:
        c.start()
    for c in copies:
        c.wait()


def solution(mesh):
    rows_size = mesh.shape["row"]
    comp_size = mesh.shape["comp"]

    def local_fit(x_local, mu_init, logpi_init, inv_temp):
        n_rows = x_local.shape[0]
        half = x_local.shape[1] // 2
        n_half = mu_init.shape[1]
        n_comp = n_half // 2
        sweeps = inv_temp.shape[0]
        total_pts = n_rows * rows_size
        n_tiles = total_pts // TILE
        tiles = n_rows // TILE
        halves = TILE // LANES
        vmem = pl.BlockSpec(memory_space=pltpu.VMEM)
        hbm = pl.BlockSpec(memory_space=pl.ANY)
        dma = pltpu.SemaphoreType.DMA
        outs = pl.pallas_call(
            functools.partial(em_kernel, sweeps, total_pts, n_half * comp_size),
            out_shape=(
                pltpu.VMEM(mu_init.shape, F32),
                pltpu.VMEM(logpi_init.shape, F32),
                pltpu.VMEM((2, n_rows), F32),
            ),
            in_specs=[hbm] * 4,
            out_specs=(vmem, vmem, vmem),
            scratch_shapes=[
                pltpu.SMEM((sweeps,), F32),
                pltpu.VMEM((n_rows, half), BF16),
                pltpu.VMEM((total_pts, half), BF16),
                pltpu.VMEM(mu_init.shape, F32),
                pltpu.VMEM(logpi_init.shape, F32),
                pltpu.VMEM((4, n_comp, half), BF16),
                pltpu.VMEM((4, n_comp, LANES), F32),
                pltpu.VMEM((2, 4, tiles, halves, LANES), F32),
                pltpu.VMEM((4, 2, n_comp, LANES), F32),
                pltpu.VMEM((2, 2, n_comp, LANES), F32),
                pltpu.VMEM((n_comp, half), BF16),
                pltpu.VMEM((n_comp, half), BF16),
                pltpu.VMEM((n_comp // LANES, LANES), F32),
                pltpu.VMEM((n_comp // LANES, LANES), F32),
                pltpu.VMEM((n_comp, half), BF16),
                pltpu.VMEM((n_comp, LANES), F32),
                pltpu.VMEM((n_tiles, n_comp, TILE), F32),
                pltpu.VMEM((n_tiles, halves, LANES), F32),
                pltpu.VMEM((sweeps - 1, 4, n_tiles, halves, LANES), F32),
                pltpu.VMEM((n_comp, total_pts), BF16),
                pltpu.VMEM((n_comp, half), F32),
                pltpu.VMEM((n_comp, LANES), F32),
                pltpu.VMEM((n_tiles, halves, LANES), F32),
                pltpu.VMEM((tiles, halves, LANES), F32),
                pltpu.VMEM((rows_size, n_comp // LANES, LANES), F32),
                dma((6,)), dma, dma, dma((3,)), dma, dma, dma((2,)), dma((3,)), dma, dma,
                dma((sweeps - 1, 2)), dma, dma((PIECES,)), dma, dma, dma,
            ],
            compiler_params=pltpu.CompilerParams(collective_id=0, has_side_effects=True),
        )(inv_temp, x_local, mu_init, logpi_init)
        outs = [pltpu.with_memory_space_constraint(o, pltpu.VMEM) for o in outs]
        return pl.pallas_call(
            store_kernel,
            out_shape=tuple(jax.ShapeDtypeStruct(o.shape, F32) for o in outs),
            in_specs=[vmem] * 3,
            out_specs=(hbm, hbm, hbm),
            scratch_shapes=[dma((3,))],
        )(*outs)

    return jax.shard_map(
        local_fit,
        mesh=mesh,
        in_specs=(P(("grp", "row"), None), P(None, ("grp", "comp"), None), P(None, ("grp", "comp")), P()),
        out_specs=(P(None, ("grp", "comp"), None), P(None, ("grp", "comp")), P(None, ("grp", "row"))),
        check_vma=False,
    )
```
